32 devices in a mesh: table: 16 (over z, y, x), dp: 2 (over core).
Axes of the slice: x: 2, y: 2, z: 4, core: 2. Of those that a mesh axis runs over, the one named last changes fastest.
Arguments:
- tables: bfloat16 [4, 65536, 128], P(None, 'table'), may hold values from -6 to 6
- owner_ids: int32 [32, 4, 256, 1], P(('table', 'dp')), may hold values from 0 to 15; in each aligned block of 256 rows (0 to 255, 256 to 511, ..., all dimensions but the last counted through in order) at most 32 rows name the same one
- row_ids: int32 [32, 4, 256], P(('table', 'dp')), may hold values from 0 to 4095
- session_of: int32 [32, 256], P(('table', 'dp')), may hold values from 0 to 1, never falling along the last dimension, each value on 1 to 200 neighbouring positions
- relevance: float32 [32, 256], P(('table', 'dp')), may hold values from 0.1 to 10
- logit_bias: float32 [32, 256], P(('table', 'dp')), may hold values from -400 to 400
- w_hidden: float32 [512, 512], replicated, may hold values from -0.25 to 0.25
- bias_hidden: float32 [512], replicated, may hold values from -3 to 3
- w_score: float32 [512], replicated, may hold values from -0.9 to 0.9
Outputs:
- emb_step: float32 [4, 65536, 128], P(None, ('table', 'dp'))
- step_hidden: float32 [512, 512], replicated
- step_bias: float32 [512], replicated
- step_score: float32 [512], replicated
- loss: float32 [], replicated
The draws below stay inside these ranges and needn't reach their ends.
Inputs may be any that keep to these rules, and one draw needn't show every extreme that they name: `owner_ids`: among one device's impressions, for one table, at most 32 name the same owner. `session_of`: session numbers never fall along a device's impressions; each of a device's 2 sessions has 1 to 200 impressions.
All inputs are finite; a program needn't handle non-finite values.
Results may differ from the reference program's by a relative error of at most 0.001.
The reference program's roundings to bfloat16 on the way (of `inputs`, `hidden_bf`, `pre_grad_bf` and `input_grad`) count: a program that leaves them out, or rounds other values in their place, can miss the bound.
Values may be sent and summed in bfloat16 or wider, within the bound.
A program may use at most 64 MiB of HBM per device.

```python
import math
import jax
import jax.numpy as jnp
import numpy as np
from jax import lax

EMB = 128
ROWS_DEV = 4096
TABLES = 4
HID = 512
SLOTS = 200
SESS_DEV = 2
IMP_DEV = 256
CAP = 32
FEAT = 512
ROWS = 65536
SESSIONS = 64
N_TABLE = 16
DEVICES = 32


def draw_logit_bias(key, part):
    key_base = jax.random.fold_in(jax.random.fold_in(key, 71), 0)
    return jnp.clip(jax.random.normal(key_base, (DEVICES, IMP_DEV), jnp.float32), -6.0, 6.0)


def with_ends(drawn, key, low, largest):
    dims = drawn.shape
    spot = [jax.random.randint(jax.random.fold_in(key, axis), (), 0, dims[axis]) for axis in range(len(dims))]
    drawn = drawn.at[tuple(spot)].set(low)
    longest = dims.index(max(dims))
    spot[longest] = (spot[longest] + 1) % dims[longest]
    return drawn.at[tuple(spot)].set(largest)


def block_levels(stream_key, dims, cuts, low, high):
    factor_of, own = 1.0, jax.random.fold_in(stream_key, 6)
    for axis_at, shards_of in cuts:
        steps = jnp.exp(jax.random.uniform(jax.random.fold_in(own, axis_at), (shards_of,), jnp.float32, low / len(cuts), high / len(cuts)))
        factor_of = factor_of * jnp.repeat(steps, dims[axis_at] // shards_of).reshape([-1 if axis == axis_at else 1 for axis in range(len(dims))])
    return factor_of


def rank_bounds(number_of, lean):
    weights = [(1 << 20) // math.isqrt(grade ** lean) + 1 for grade in range(1, number_of + 1)]
    deviation = 1 + sum(weights) // (1 << 30)
    return np.cumsum(np.array([max(1, weight // deviation) for weight in weights]))


def skewed_ids(rng, shape, count, lean):
    table = rank_bounds(count, lean)
    pick = jax.random.randint(jax.random.fold_in(rng, 1), shape, 0, int(table[count - 1]))
    rank = jnp.searchsorted(jnp.asarray(table, jnp.int32), pick, side="right")
    return jax.random.permutation(jax.random.fold_in(rng, 2), count)[rank].astype(jnp.int32)


def split_up(number_of, total, bound, skew):
    portions = [(1 << 20) // math.isqrt(rank ** skew) + 1 for rank in range(2, number_of + 1)]
    surplus, counts = total - bound - (number_of - 1), [1] * (number_of - 1)
    while surplus > 0:
        movable = [i for i in range(number_of - 1) if counts[i] < bound]
        pool, left = sum([portions[i] for i in movable]), surplus
        for i in movable:
            addition = min(bound - counts[i], max(1, left * portions[i] // pool), surplus)
            counts[i] = counts[i] + addition
            surplus = surplus - addition
    return np.array([bound] + counts)


def ragged(own_key, number_of, total, most, slope):
    if number_of == 2:
        one = jax.random.randint(own_key, (), max(1, total - most), min(most, total - 1) + 1)
        return jnp.stack([one, total - one])
    sizes = jnp.asarray(split_up(number_of, total, most, slope), jnp.int32)
    couples = (number_of - 1) // 2
    donor, receiver = sizes[1:1 + 2 * couples:2], sizes[2:2 + 2 * couples:2]
    room = jnp.minimum(donor - 1, most - receiver)
    moved = jax.random.randint(jax.random.fold_in(own_key, 1), (couples,), 0, 1 << 20) % (room + 1)
    sizes = sizes.at[1:1 + 2 * couples:2].set(donor - moved).at[2:2 + 2 * couples:2].set(receiver + moved)
    return sizes[jax.random.permutation(jax.random.fold_in(own_key, 2), number_of)]


def assign_block(own_key, own, number, rows, count, top, limit, slope):
    ranking = jax.random.permutation(own_key, count)
    heavy_load, usual = portions_of(count, rows * top, limit, slope, True), portions_of(count, rows * top, limit, slope, False)
    places = jnp.arange(count)

    def named(lengths, rotation):
        used = int((lengths > 0).sum())
        fixed = max(1, used // 4)
        moved = fixed + (places - fixed + rotation * (used - fixed)) % max(1, count - fixed)
        return jnp.zeros((count,), jnp.int32).at[ranking[jnp.where(places < fixed, places, moved)]].set(jnp.asarray(lengths, jnp.int32))

    lengths = jnp.where(number % 4 == 0, named(heavy_load, number // 4), named(usual, number - number // 4 - 1))
    mixed = jax.random.permutation(jax.random.fold_in(own, 3), count)
    giver, sink = mixed[0:count // 2 * 2:2], mixed[1:count // 2 * 2:2]
    room = jnp.minimum(lengths[giver] - 1, limit - lengths[sink]) // 2
    room = jnp.where((giver == ranking[0]) | (sink == ranking[0]) | (lengths[sink] == 0), 0, jnp.maximum(room, 0))
    moved = jax.random.randint(jax.random.fold_in(own, 4), (count // 2,), 0, 1 << 20) % (room + 1)
    lengths = lengths.at[giver].add(-moved).at[sink].add(moved)
    labels = jnp.searchsorted(jnp.cumsum(lengths), jnp.arange(rows * top), side="right").astype(jnp.int32)
    grid = labels.reshape(top, rows).T
    grid = grid[jax.random.permutation(jax.random.fold_in(own, 1), rows)]
    rotation = jax.random.randint(jax.random.fold_in(own, 2), (rows, 1), 0, top)
    return jnp.take_along_axis(grid, (jnp.arange(top)[None, :] + rotation) % top, axis=1)


def portions_of(amount, total, reach, slope, full):
    loads = [(1 << 20) // math.isqrt(rank ** slope) + 1 for rank in range(1, amount + 1)]
    largest = reach if full else min(reach, max(-(-total // amount), total * loads[0] // sum(loads)))
    least = 1 if total - largest >= amount - 1 else 0
    counts, surplus = [largest] + [least] * (amount - 1), total - largest - least * (amount - 1)
    while surplus > 0:
        candidates = [i for i in range(1, amount) if counts[i] < largest] or [i for i in range(1, amount) if counts[i] < reach]
        pool, left = sum([loads[i] for i in candidates]), surplus
        for i in candidates:
            more = min(reach - counts[i], max(1, left * loads[i] // pool), surplus)
            counts[i] = counts[i] + more
            surplus = surplus - more
    return np.array(counts)


def normal_values(rng, extent, spread, most, cuts=(), kind=jnp.bfloat16):
    array = jax.random.normal(rng, extent, jnp.float32) * spread
    if len(cuts) > 0:
        array = block_levels(rng, extent, cuts, -0.22, 0.18) * array
    return jnp.clip(array, min=-most, max=most).astype(kind)


def setup_inputs(seed: int = 0) -> dict:
    streams_of = jax.random.split(jax.random.key(seed), 10)
    tables = normal_values(streams_of[0], (TABLES, ROWS, EMB), 1.0, 6.0, ((1, 16),))
    owner_ids_keys = jax.random.split(jax.random.fold_in(streams_of[1], 1), DEVICES * TABLES * IMP_DEV // IMP_DEV)
    owner_ids_turns = jax.random.permutation(jax.random.fold_in(streams_of[1], 3), DEVICES * TABLES * IMP_DEV // IMP_DEV)
    owner_ids = jax.vmap(lambda own, number: assign_block(jax.random.fold_in(streams_of[1], 2), own, number, IMP_DEV, N_TABLE, 1, CAP, 1))(owner_ids_keys, owner_ids_turns).reshape((DEVICES, TABLES, IMP_DEV, 1))
    row_ids = with_ends(skewed_ids(streams_of[2], (DEVICES, TABLES, IMP_DEV), ROWS_DEV, 2), jax.random.fold_in(streams_of[2], 3), 0, ROWS_DEV - 1).astype(jnp.int32)
    session_of = jax.vmap(lambda own: jnp.searchsorted(jnp.cumsum(ragged(own, SESS_DEV, IMP_DEV, SLOTS, 1)), jnp.arange(IMP_DEV), side="right"))(jax.random.split(streams_of[3], DEVICES)).reshape((DEVICES, IMP_DEV)).astype(jnp.int32)
    relevance = jnp.clip(jnp.exp(math.log(10.0) - 4.6051702 * jax.random.uniform(streams_of[4], (DEVICES, IMP_DEV), jnp.float32) ** block_levels(streams_of[4], (DEVICES, IMP_DEV), ((0, 32),), -0.2, 0.2)), 0.1, 10.0)
    logit_bias = draw_logit_bias(jax.random.fold_in(streams_of[9], 71), 0)
    w_hidden = normal_values(streams_of[6], (FEAT, HID), FEAT ** -0.5, 0.25, (), jnp.float32)
    bias_hidden = normal_values(streams_of[7], (HID,), 0.5, 3.0, (), jnp.float32)
    w_score = normal_values(streams_of[8], (HID,), 0.15, 0.9, (), jnp.float32)
    return {"tables": tables, "owner_ids": owner_ids, "row_ids": row_ids, "session_of": session_of, "relevance": relevance, "logit_bias": logit_bias, "w_hidden": w_hidden, "bias_hidden": bias_hidden, "w_score": w_score}


def silu_slope(pre_val):
    logistic = jax.nn.sigmoid(pre_val)
    return logistic * (1.0 + pre_val * (1.0 - logistic))

def session_terms(scores, session_ids, relevance, sessions):
    member = session_ids[None, :] == jnp.arange(sessions, dtype=jnp.int32)[:, None]
    highest = lax.optimization_barrier(jnp.max(jnp.where(member, scores[None, :], -jnp.inf), axis=1))
    highest_each = lax.optimization_barrier(jnp.sum(jnp.where(member, highest[:, None], 0.0), axis=0))
    shifted = scores - highest_each
    exponent = jnp.exp(shifted)
    totals = lax.optimization_barrier(jnp.sum(jnp.where(member, exponent[None, :], 0.0), axis=1))
    weights = lax.optimization_barrier(jnp.sum(jnp.where(member, relevance[None, :], 0.0), axis=1))
    total_each = lax.optimization_barrier(jnp.sum(jnp.where(member, totals[:, None], 0.0), axis=0))
    weight_each = lax.optimization_barrier(jnp.sum(jnp.where(member, weights[:, None], 0.0), axis=0))
    probability = exponent / total_each
    target = relevance / weight_each
    loss_sum = jnp.sum(jnp.log(totals)) - jnp.sum(target * shifted)
    return (loss_sum, probability - target)

def reference(tables, owner_ids, row_ids, session_of, relevance, logit_bias, w_hidden, bias_hidden, w_score):
    hidden_bf = w_hidden.astype(jnp.bfloat16)
    global_rows = owner_ids[:, :, :, 0] * ROWS_DEV + row_ids
    table_index = jnp.arange(TABLES, dtype=jnp.int32)

    def block_step(carry, block):
        weight_acc, bias_acc, score_acc, loss_acc = carry
        rows_here, session_ids, relevant, bias_row = block
        fetched = tables[table_index[None, :], rows_here.T]
        inputs = fetched.reshape(IMP_DEV, TABLES * EMB)
        pre_act = jnp.dot(inputs, hidden_bf, preferred_element_type=jnp.float32) + bias_hidden
        hidden = jax.nn.silu(pre_act)
        scores = jnp.dot(hidden, w_score, precision=lax.Precision.HIGHEST) + bias_row
        loss_sum, score_grad = session_terms(scores, session_ids, relevant, SESS_DEV)
        pre_grad = score_grad[:, None] * w_score[None, :] * silu_slope(pre_act)
        pre_grad_bf = pre_grad.astype(jnp.bfloat16)
        weight_grad = lax.dot_general(inputs, pre_grad_bf, (((0,), (0,)), ((), ())), preferred_element_type=jnp.float32)
        bias_grad = lax.optimization_barrier(jnp.sum(pre_grad, axis=0))
        score_weight_grad = jnp.dot(score_grad, hidden, precision=lax.Precision.HIGHEST)
        input_grad = jnp.dot(pre_grad_bf, hidden_bf.T, preferred_element_type=jnp.float32).astype(jnp.bfloat16)
        carry = (weight_acc + weight_grad, bias_acc + bias_grad, score_acc + score_weight_grad, loss_acc + loss_sum)
        return (carry, input_grad.reshape(IMP_DEV, TABLES, EMB))
    init = (jnp.zeros((FEAT, HID), jnp.float32), jnp.zeros((HID,), jnp.float32), jnp.zeros((HID,), jnp.float32), jnp.zeros((), jnp.float32))
    totals, grads = lax.scan(block_step, init, (global_rows, session_of, relevance, logit_bias))
    weight_tot, bias_tot, score_tot, loss_tot = totals
    row_grad = jnp.zeros((TABLES, ROWS, EMB), jnp.float32)
    row_grad = row_grad.at[table_index[None, None, :], jnp.transpose(global_rows, (0, 2, 1))].add(grads.astype(jnp.float32))
    emb_step = row_grad / (jnp.sqrt(lax.optimization_barrier(jnp.mean(row_grad * row_grad, axis=2, keepdims=True))) + 1e-06)
    param_count = FEAT * HID + 2 * HID
    mean_sq = (jnp.sum(weight_tot * weight_tot) + jnp.sum(bias_tot * bias_tot) + jnp.sum(score_tot * score_tot)) / param_count
    factor = 1.0 / jnp.sqrt(mean_sq + 1e-06)
    loss = loss_tot / SESSIONS
    return (emb_step, weight_tot * factor, bias_tot * factor, score_tot * factor, loss)
```

```python
import jax
import jax.numpy as jnp
from jax import lax
from jax.experimental import pallas as pl
from jax.experimental.pallas import tpu as pltpu
import functools
from jax.sharding import PartitionSpec as P

SESS_DEV = 2


def silu_slope(pre_val):
    logistic = jax.nn.sigmoid(pre_val)
    return logistic * (1.0 + pre_val * (1.0 - logistic))


def session_terms(scores, session_ids, relevance, sessions):
    member = session_ids[None, :] == jnp.arange(sessions, dtype=jnp.int32)[:, None]
    highest = jnp.max(jnp.where(member, scores[None, :], -jnp.inf), axis=1)
    highest_each = jnp.sum(jnp.where(member, highest[:, None], 0.0), axis=0)
    shifted = scores - highest_each
    exponent = jnp.exp(shifted)
    totals = jnp.sum(jnp.where(member, exponent[None, :], 0.0), axis=1)
    weights = jnp.sum(jnp.where(member, relevance[None, :], 0.0), axis=1)
    total_each = jnp.sum(jnp.where(member, totals[:, None], 0.0), axis=0)
    weight_each = jnp.sum(jnp.where(member, weights[:, None], 0.0), axis=0)
    probability = exponent / total_each
    target = relevance / weight_each
    loss_sum = jnp.sum(jnp.log(totals)) - jnp.sum(target * shifted)
    return (loss_sum, probability - target)


def selector(indices, count):
    return (indices[:, None] == jnp.arange(count, dtype=jnp.int32)[None, :]).astype(jnp.bfloat16)


def pick_rows(indices, source):
    return jnp.dot(
        selector(indices, source.shape[0]), source, preferred_element_type=jnp.float32
    ).astype(jnp.bfloat16)


def place_rows(indices, values, count):
    return lax.dot_general(
        selector(indices, count),
        values,
        (((0,), (0,)), ((), ())),
        preferred_element_type=jnp.float32,
    )


def on_device(
    tables, owner_ids, row_ids, session_of, relevance, logit_bias, w_hidden, bias_hidden, w_score
):
    owners = lax.axis_size("table")
    devices = owners * lax.axis_size("dp")
    table_count, shard_rows, emb_width = tables.shape
    owner_now = owner_ids[0, :, :, 0]
    rows_now = row_ids[0]
    imp_count = owner_now.shape[1]
    capacity = 2 * imp_count // owners
    slot_total = owners * capacity
    one_hot = (owner_now[:, :, None] == jnp.arange(owners, dtype=jnp.int32)).astype(jnp.float32)
    places = jnp.arange(imp_count, dtype=jnp.int32)
    lower_tri = (places[:, None] >= places[None, :]).astype(jnp.float32)
    running = jnp.einsum("ij,tjo->tio", lower_tri, one_hot, precision=lax.Precision.HIGHEST)
    rank_in = (jnp.sum(running * one_hot, axis=2) - 1.0).astype(jnp.int32)
    slot_of = owner_now * capacity + rank_in
    slot_hot = (slot_of[:, :, None] == jnp.arange(slot_total, dtype=jnp.int32)).astype(jnp.int32)
    wanted = jnp.sum(slot_hot * rows_now[:, :, None], axis=1) + shard_rows * (
        1 - jnp.sum(slot_hot, axis=1)
    )
    if (
        capacity % 16 == 0
        and table_count * capacity == 128
        and w_hidden.shape[0] == w_hidden.shape[1]
    ):
        return whole_kernel(
            tables,
            jnp.transpose(wanted.reshape(table_count, owners, capacity), (1, 0, 2)),
            slot_of,
            session_of[0],
            relevance[0],
            logit_bias[0],
            w_hidden,
            bias_hidden,
            w_score,
        )
    requested = lax.all_to_all(
        wanted.reshape(table_count, owners, capacity),
        "table",
        split_axis=1,
        concat_axis=1,
        tiled=True,
    )
    served = lax.map(
        lambda pair: pick_rows(pair[0], pair[1]),
        (requested.reshape(table_count, slot_total), tables),
    )
    served = served.reshape(table_count, owners, capacity, emb_width)
    hidden_bf = w_hidden.astype(jnp.bfloat16)
    returned = lax.all_to_all(served, "table", split_axis=1, concat_axis=1, tiled=True).reshape(
        table_count, slot_total, emb_width
    )
    gathered = lax.map(lambda pair: pick_rows(pair[0], pair[1]), (slot_of, returned))
    inputs = jnp.transpose(gathered, (1, 0, 2)).reshape(imp_count, table_count * emb_width)
    pre_act = jnp.dot(inputs, hidden_bf, preferred_element_type=jnp.float32)
    pre_act = pre_act + bias_hidden
    hidden = jax.nn.silu(pre_act)
    scores = jnp.dot(hidden, w_score, precision=lax.Precision.HIGHEST) + logit_bias[0]
    loss_sum, score_grad = session_terms(scores, session_of[0], relevance[0], SESS_DEV)
    pre_grad = score_grad[:, None] * w_score[None, :] * silu_slope(pre_act)
    pre_grad_bf = pre_grad.astype(jnp.bfloat16)
    weight_grad = lax.dot_general(
        inputs, pre_grad_bf, (((0,), (0,)), ((), ())), preferred_element_type=jnp.float32
    )
    bias_grad = jnp.sum(pre_grad, axis=0)
    score_weight_grad = jnp.dot(score_grad, hidden, precision=lax.Precision.HIGHEST)
    input_grad = jnp.dot(pre_grad_bf, hidden_bf.T, preferred_element_type=jnp.float32).astype(
        jnp.bfloat16
    )
    input_grad = jnp.transpose(input_grad.reshape(imp_count, table_count, emb_width), (1, 0, 2))
    outgoing = lax.map(
        lambda pair: place_rows(pair[0], pair[1], slot_total).astype(jnp.bfloat16),
        (slot_of, input_grad),
    )
    incoming = lax.all_to_all(
        outgoing.reshape(table_count, owners, capacity, emb_width),
        "table",
        split_axis=1,
        concat_axis=1,
        tiled=True,
    )
    summed = lax.map(
        lambda pair: place_rows(pair[0], pair[1], shard_rows),
        (
            requested.reshape(table_count, slot_total),
            incoming.reshape(table_count, slot_total, emb_width),
        ),
    )
    own_rows = lax.psum_scatter(summed, "dp", scatter_dimension=1, tiled=True)
    emb_step = own_rows / (jnp.sqrt(jnp.mean(own_rows * own_rows, axis=2, keepdims=True)) + 1e-06)
    param_count = w_hidden.size + bias_hidden.size + w_score.size
    weight_tot, bias_tot, score_tot, loss_tot = lax.psum(
        (weight_grad, bias_grad, score_weight_grad, loss_sum), ("table", "dp")
    )
    mean_sq = (
        jnp.sum(weight_tot * weight_tot)
        + jnp.sum(bias_tot * bias_tot)
        + jnp.sum(score_tot * score_tot)
    ) / param_count
    factor = 1.0 / jnp.sqrt(mean_sq + 1e-06)
    step_hidden = weight_tot * factor
    loss = loss_tot / (SESS_DEV * devices)
    return (emb_step, step_hidden, bias_tot * factor, score_tot * factor, loss)


MESH = pl.DeviceIdType.MESH


def whole_body(
    sizes, tables_hbm, wanted_ref, slots_ref, columns_ref, weights_ref, bias_ref, scorer_ref,
    emb_rows, step_ref, small_ref,
    tables_ref, ids_in, ids_ref, served, picked, picked_rows, gathered, dense_ref, out_ref,
    load_sem, want_sems, want_own, serve_send, serve_recv, serve_own, grads, swapped, ids_other, from_other, from_plane, from_column, sum_pair, sum_plane,
    total, grad_send, grad_recv, own_sem, swap_send, swap_recv, ids_sems, pair_sems, plane_send,
    plane_recv, column_send, column_recv,
):
    tables, owners, capacity, width, half_rows, inner, outer, hid, sessions, own_sessions = sizes
    slots = owners * capacity
    me = lax.axis_index("table")
    core = lax.axis_index("dp")
    low, high = lax.rem(me, inner), me // inner
    other = (me, 1 - core)

    def load(table):
        return pltpu.make_async_copy(
            tables_hbm.at[table], tables_ref.at[table], load_sem.at[table]
        )

    for table in range(tables):
        load(table).start()
    barrier = pltpu.get_barrier_semaphore()

    def greet(step, carry):
        pl.semaphore_signal(
            barrier, inc=1, device_id=(lax.rem(me + step, owners), core), device_id_type=MESH
        )
        return carry

    pl.semaphore_signal(barrier, inc=1, device_id=other, device_id_type=MESH)
    lax.fori_loop(1, owners, greet, 0)
    pl.semaphore_wait(barrier, owners)

    def remote(src, dst, send, recv, to):
        return pltpu.make_async_remote_copy(
            src_ref=src, dst_ref=dst, send_sem=send, recv_sem=recv, device_id=to,
            device_id_type=MESH,
        )

    def to_peers(copy_to):
        def one(step, carry):
            copy_to(lax.rem(me + step, owners)).start()
            return carry

        lax.fori_loop(1, owners, one, 0)

    to_peers(
        lambda peer: remote(
            wanted_ref.at[peer], ids_in.at[me], want_sems.at[0], want_sems.at[1], (peer, core)
        )
    )
    want_mine = pltpu.make_async_copy(wanted_ref.at[me], ids_in.at[me], want_own.at[0])
    want_mine.start()
    w_bf = weights_ref[...].astype(jnp.bfloat16)
    want_mine.wait()
    remote(
        wanted_ref.at[pl.ds(0, owners - 1)], ids_in.at[pl.ds(0, owners - 1)], want_sems.at[0],
        want_sems.at[1], other,
    ).wait()

    depth = 1024
    shard_rows = 2 * half_rows

    def serve_own_copy(table):
        return pltpu.make_async_copy(
            served.at[table, me], picked.at[table, me], serve_own.at[table]
        )

    for table in range(tables):
        named = jnp.broadcast_to(
            ids_in[:, 0:1, :].astype(jnp.float32), (owners, capacity, 128)
        )
        lane = lax.broadcasted_iota(jnp.int32, named.shape, 2)
        place_in = lax.broadcasted_iota(jnp.int32, named.shape, 1) + table * capacity
        wide_ids = jnp.broadcast_to(
            jnp.sum(jnp.where(lane == place_in, named, 0.0), axis=2, keepdims=True), named.shape
        ).reshape(slots, 128).astype(jnp.int32)
        ids_ref[pl.ds(table, 1), :] = wide_ids.T[0:1, :]
        ids_col = wide_ids[:, 0:1]
        load(table).wait()
        picked_rows[...] = jnp.zeros_like(picked_rows)

        def pick_block(step, carry):
            at = lax.broadcasted_iota(jnp.int32, (slots, depth), 1)
            hot = jnp.where(at == ids_col - step * depth, 1.0, 0.0).astype(jnp.bfloat16)
            rows_at = pl.ds(pl.multiple_of(step * depth, depth), depth)
            picked_rows[...] += jnp.dot(
                hot, tables_ref[table, rows_at, :], preferred_element_type=jnp.float32
            )
            return carry

        lax.fori_loop(0, shard_rows // depth, pick_block, 0)
        served[table] = picked_rows[...].astype(jnp.bfloat16).reshape(owners, capacity, width)
        serve_own_copy(table).start()
        to_peers(
            lambda peer, table=table: remote(
                served.at[table, peer], picked.at[table, me], serve_send.at[table],
                serve_recv.at[table], (peer, core),
            )
        )
    ids_copy = remote(ids_ref, ids_other, ids_sems.at[0], ids_sems.at[1], other)
    ids_copy.start()

    imps = gathered.shape[0]
    for table in range(tables):
        serve_own_copy(table).wait()
        remote(
            served.at[table, pl.ds(0, owners - 1)], picked.at[table, pl.ds(0, owners - 1)],
            serve_send.at[table], serve_recv.at[table], other,
        ).wait()
        slot_col = columns_ref[:, table : table + 1].astype(jnp.int32)
        hot = jnp.where(
            lax.broadcasted_iota(jnp.int32, (imps, slots), 1) == slot_col, 1.0, 0.0
        ).astype(jnp.bfloat16)
        gathered[:, table * width : (table + 1) * width] = jnp.dot(
            hot, picked[table].reshape(slots, width), preferred_element_type=jnp.float32
        ).astype(jnp.bfloat16)
    inputs = gathered[...]
    pre_act = jnp.dot(inputs, w_bf, preferred_element_type=jnp.float32) + bias_ref[...]
    logistic = 1.0 / (1.0 + jnp.exp(-pre_act))
    hidden = pre_act * logistic
    session = columns_ref[:, tables : tables + 1].astype(jnp.int32)
    relevance = columns_ref[:, tables + 1 : tables + 2]
    scores = jnp.sum(hidden * scorer_ref[...], axis=1, keepdims=True)
    scores = scores + columns_ref[:, tables + 2 : tables + 3]
    member = lax.broadcasted_iota(jnp.int32, (imps, 128), 1) == session
    highest = jnp.max(jnp.where(member, scores, -jnp.inf), axis=0, keepdims=True)
    highest_each = jnp.sum(jnp.where(member, highest, 0.0), axis=1, keepdims=True)
    shifted = scores - highest_each
    exponent = jnp.exp(shifted)
    totals = jnp.sum(jnp.where(member, exponent, 0.0), axis=0, keepdims=True)
    weights = jnp.sum(jnp.where(member, relevance, 0.0), axis=0, keepdims=True)
    total_each = jnp.sum(jnp.where(member, totals, 0.0), axis=1, keepdims=True)
    weight_each = jnp.sum(jnp.where(member, weights, 0.0), axis=1, keepdims=True)
    target = relevance / weight_each
    real = lax.broadcasted_iota(jnp.int32, (1, 128), 1) < own_sessions
    loss_sum = jnp.sum(jnp.log(jnp.where(real, totals, 1.0)), keepdims=True) - jnp.sum(
        target * shifted, keepdims=True
    )
    score_grad = exponent / total_each - target
    pre_grad = score_grad * scorer_ref[...] * (logistic * (1.0 + pre_act * (1.0 - logistic)))
    pre_grad_bf = pre_grad.astype(jnp.bfloat16)
    weight_grad = lax.dot_general(
        inputs, pre_grad_bf, (((0,), (0,)), ((), ())), preferred_element_type=jnp.float32
    )
    bias_grad = jnp.sum(pre_grad, axis=0, keepdims=True)
    score_weight_grad = jnp.sum(score_grad * hidden, axis=0, keepdims=True)
    line = lax.broadcasted_iota(jnp.int32, (128, hid), 0)
    spot = lax.broadcasted_iota(jnp.int32, (128, hid), 1)
    extra = jnp.where(line == 0, bias_grad, 0.0) + jnp.where(line == 1, score_weight_grad, 0.0)
    extra = extra + jnp.where((line == 2) & (spot == 0), loss_sum, 0.0)
    dense_ref[:, :, :, :, :hid] = weight_grad.reshape(dense_ref.shape[:4] + (hid,))
    dense_ref[:, :, :, :, hid:] = extra.T.reshape(dense_ref.shape[:4] + (128,))
    pair_up = remote(dense_ref.at[1 - core], from_other, pair_sems.at[0], pair_sems.at[1], other)
    pair_up.start()
    input_grad = lax.dot_general(
        pre_grad_bf, w_bf, (((1,), (1,)), ((), ())), preferred_element_type=jnp.float32
    ).astype(jnp.bfloat16)

    def fill(table):
        hot = jnp.where(
            lax.broadcasted_iota(jnp.int32, (slots, imps), 0) == slots_ref[pl.ds(table, 1), :],
            1.0, 0.0,
        ).astype(jnp.bfloat16)
        out_ref[table] = jnp.dot(
            hot, input_grad[:, table * width : (table + 1) * width],
            preferred_element_type=jnp.float32,
        ).astype(jnp.bfloat16).reshape(owners, capacity, width)

    def own_copy(table):
        return pltpu.make_async_copy(
            out_ref.at[table, me], grads.at[table, me], own_sem.at[table]
        )

    def send_grads(table):
        fill(table)
        own_copy(table).start()

        def send_one(step, carry):
            owner = lax.rem(me + step, owners)
            remote(
                out_ref.at[table, owner], grads.at[table, me], grad_send.at[table],
                grad_recv.at[table], (owner, core),
            ).start()
            return carry

        lax.fori_loop(1, owners, send_one, 0)

    def all_grads(table):
        return remote(
            out_ref.at[table, pl.ds(0, owners - 1)], grads.at[table, pl.ds(0, owners - 1)],
            grad_send.at[table], grad_recv.at[table], other,
        )

    def swap(table):
        return remote(
            grads.at[table], swapped.at[table], swap_send.at[table], swap_recv.at[table], other
        )

    def arrive(table):
        own_copy(table).wait()
        all_grads(table).wait()
        swap(table).start()

    block = 256


    def place(table):
        swap(table).wait()
        ids_mine = ids_ref[pl.ds(table, 1), :]
        ids_theirs = ids_other[pl.ds(table, 1), :]
        rows_mine = grads[table].reshape(slots, width)
        rows_theirs = swapped[table].reshape(slots, width)

        def place_block(step, carry):
            at = lax.broadcasted_iota(jnp.int32, (block, slots), 0) + (
                core * half_rows + step * block
            )
            hot_mine = jnp.where(at == ids_mine, 1.0, 0.0).astype(jnp.bfloat16)
            hot_theirs = jnp.where(at == ids_theirs, 1.0, 0.0).astype(jnp.bfloat16)
            summed = jnp.dot(hot_mine, rows_mine, preferred_element_type=jnp.float32)
            summed = summed + jnp.dot(hot_theirs, rows_theirs, preferred_element_type=jnp.float32)
            mean = jnp.sum(summed * summed, axis=1, keepdims=True) / width
            emb_rows[table, pl.ds(pl.multiple_of(step * block, block), block), :] = summed / (
                jnp.sqrt(mean) + 1e-06
            )
            return carry

        lax.fori_loop(0, half_rows // block, place_block, 0)

    def plane_copies(phase, src_of, dst_of):
        return [
            remote(
                src_of(lax.rem(low + step, inner)), dst_of(step - 1), plane_send.at[phase, step - 1],
                plane_recv.at[phase, step - 1], (high * inner + lax.rem(low + step, inner), core),
            )
            for step in range(1, inner)
        ]

    def column_copies(phase, src_of, dst_of):
        return [
            remote(
                src_of(lax.rem(high + step, outer)), dst_of(step - 1), column_send.at[phase, step - 1],
                column_recv.at[phase, step - 1], (lax.rem(high + step, outer) * inner + low, core),
            )
            for step in range(1, outer)
        ]

    def run(copies):
        for copy in copies:
            copy.start()

    def finish(copies):
        for copy in copies:
            copy.wait()

    send_grads(0)
    pair_up.wait()
    sum_pair[...] = dense_ref[core] + from_other[...]
    plane_sum = plane_copies(0, lambda to: sum_pair.at[to], lambda slot: from_plane.at[slot])
    run(plane_sum)
    for table in range(1, tables):
        send_grads(table)
    ids_copy.wait()
    finish(plane_sum)
    part = sum_pair[low]
    for slot in range(inner - 1):
        part = part + from_plane[slot]
    sum_plane[...] = part
    column_sum = column_copies(0, lambda to: sum_plane.at[to], lambda slot: from_column.at[slot])
    run(column_sum)
    arrive(0)
    finish(column_sum)
    part = sum_plane[high]
    for slot in range(outer - 1):
        part = part + from_column[slot]
    total[core, low, high] = part
    column_share = column_copies(
        1, lambda to: total.at[core, low, high], lambda slot: total.at[core, low, high]
    )
    run(column_share)
    place(0)
    for table in range(1, tables):
        if table == 1:
            finish(column_share)
            plane_share = plane_copies(
                1, lambda to: total.at[core, low], lambda slot: total.at[core, low]
            )
            run(plane_share)
        arrive(table)
        if table == tables - 1:
            finish(plane_share)
            pair_down = remote(
                total.at[core], total.at[core], pair_sems.at[2], pair_sems.at[3], other
            )
            pair_down.start()
        place(table)
    pair_down.wait()
    every = total[...].reshape(2 * owners * dense_ref.shape[3], dense_ref.shape[4])
    weights, extra = every[:, :hid], every[:, hid:]
    counted = lax.broadcasted_iota(jnp.int32, extra.shape, 1) < 2
    counts = jnp.where(counted, extra, 0.0)
    squares = jnp.sum(weights * weights, keepdims=True) + jnp.sum(counts * counts, keepdims=True)
    factor = 1.0 / jnp.sqrt(squares / (hid * hid + 2 * hid) + 1e-06)
    step_ref[...] = weights * factor
    scaled = jnp.where(counted, extra * factor, extra / sessions)
    small_ref[...] = scaled.T


def write_body(
    rows_ref, weights_ref, small_ref, emb_ref, hidden_ref, bias_ref, score_ref, loss_ref, sems
):
    copies = [
        pltpu.make_async_copy(rows_ref.at[table], emb_ref.at[table], sems.at[table])
        for table in range(rows_ref.shape[0])
    ]
    for copy in copies:
        copy.start()
    hidden_ref[...] = weights_ref[...]
    bias_ref[...] = small_ref[0:1, :]
    score_ref[...] = small_ref[1:2, :]
    loss_ref[...] = small_ref[2:3, 0:1]
    for copy in copies:
        copy.wait()


def whole_kernel(
    tables, wanted, slot_of, session, relevance, logit_bias, w_hidden, bias_hidden, w_score
):
    table_count, shard_rows, width = tables.shape
    owners, _, capacity = wanted.shape
    hid = w_hidden.shape[1]
    imps = session.shape[0]
    slots = owners * capacity
    half_rows = shard_rows // 2
    inner = 1
    while inner * inner < owners:
        inner *= 2
    outer = owners // inner
    rows = hid // (2 * owners)
    wide = hid + 128
    wanted = jnp.broadcast_to(
        wanted.reshape(owners, 1, table_count * capacity), (owners, 8, table_count * capacity)
    )
    columns = jnp.stack(
        [slot_of[table].astype(jnp.float32) for table in range(table_count)]
        + [session.astype(jnp.float32), relevance, logit_bias],
        axis=1,
    )
    sizes = (
        table_count, owners, capacity, width, half_rows, inner, outer, hid,
        SESS_DEV * owners * 2, SESS_DEV,
    )
    f32, bf16 = jnp.float32, jnp.bfloat16
    dma = pltpu.SemaphoreType.DMA
    vmem = pl.BlockSpec(memory_space=pltpu.VMEM)
    emb_step, step_hidden, small = pl.pallas_call(
        functools.partial(whole_body, sizes),
        out_shape=(
            jax.ShapeDtypeStruct((table_count, half_rows, width), f32),
            jax.ShapeDtypeStruct((hid, hid), f32),
            jax.ShapeDtypeStruct((128, hid), f32),
        ),
        in_specs=[pl.BlockSpec(memory_space=pl.ANY)] + [vmem] * 6,
        out_specs=(vmem, vmem, vmem),
        scratch_shapes=[
            pltpu.VMEM(tables.shape, bf16),
            pltpu.VMEM(wanted.shape, jnp.int32),
            pltpu.VMEM((table_count, slots), jnp.int32),
            pltpu.VMEM((table_count, owners, capacity, width), bf16),
            pltpu.VMEM((table_count, owners, capacity, width), bf16),
            pltpu.VMEM((slots, width), f32),
            pltpu.VMEM((imps, table_count * width), bf16),
            pltpu.VMEM((2, inner, outer, rows, wide), f32),
            pltpu.VMEM((table_count, owners, capacity, width), bf16),
            dma((table_count,)), dma((2,)), dma((1,)),
            dma((table_count,)), dma((table_count,)), dma((table_count,)),
            pltpu.VMEM((table_count, owners, capacity, width), bf16),
            pltpu.VMEM((table_count, owners, capacity, width), bf16),
            pltpu.VMEM((table_count, slots), jnp.int32),
            pltpu.VMEM((inner, outer, rows, wide), f32),
            pltpu.VMEM((inner - 1, outer, rows, wide), f32),
            pltpu.VMEM((outer - 1, rows, wide), f32),
            pltpu.VMEM((inner, outer, rows, wide), f32),
            pltpu.VMEM((outer, rows, wide), f32),
            pltpu.VMEM((2, inner, outer, rows, wide), f32),
            dma((table_count,)), dma((table_count,)), dma((table_count,)),
            dma((table_count,)), dma((table_count,)),
            dma((2,)), dma((4,)),
            dma((2, inner - 1)), dma((2, inner - 1)), dma((2, outer - 1)), dma((2, outer - 1)),
        ],
        compiler_params=pltpu.CompilerParams(
            collective_id=1, has_side_effects=True, vmem_limit_bytes=36 * 1024 * 1024
        ),
    )(tables, wanted, slot_of, columns, w_hidden, bias_hidden[None, :], w_score[None, :])
    emb_step, step_hidden, b, c, d = pl.pallas_call(write_body, out_shape=(jax.ShapeDtypeStruct((table_count, half_rows, width), f32),
            jax.ShapeDtypeStruct((hid, hid), f32),jax.ShapeDtypeStruct((1, hid), f32),jax.ShapeDtypeStruct((1, hid), f32),jax.ShapeDtypeStruct((1, 1), f32)),
            in_specs=[vmem]*3, out_specs=(pl.BlockSpec(memory_space=pl.ANY),vmem,vmem,vmem,vmem), scratch_shapes=[dma((table_count,))],
            compiler_params=pltpu.CompilerParams(vmem_limit_bytes=8*1024*1024))(emb_step, step_hidden, small)
    return (emb_step, step_hidden, b[0], c[0], d[0, 0])


def solution(mesh):
    in_specs = (
        P(None, "table", None),
        P(("table", "dp"), None, None, None),
        P(("table", "dp"), None, None),
        P(("table", "dp"), None),
        P(("table", "dp"), None),
        P(("table", "dp"), None),
        P(),
        P(),
        P(),
    )
    out_specs = (P(None, ("table", "dp"), None), P(), P(), P(), P())
    return jax.shard_map(
        on_device, mesh=mesh, in_specs=in_specs, out_specs=out_specs, check_vma=False
    )
```

```python
import jax
import jax.numpy as jnp
from jax import lax
from jax.experimental import pallas as pl
from jax.experimental.pallas import tpu as pltpu
import functools
from jax.sharding import PartitionSpec as P

SESS_DEV = 2


def silu_slope(pre_val):
    logistic = jax.nn.sigmoid(pre_val)
    return logistic * (1.0 + pre_val * (1.0 - logistic))


def session_terms(scores, session_ids, relevance, sessions):
    member = session_ids[None, :] == jnp.arange(sessions, dtype=jnp.int32)[:, None]
    highest = jnp.max(jnp.where(member, scores[None, :], -jnp.inf), axis=1)
    highest_each = jnp.sum(jnp.where(member, highest[:, None], 0.0), axis=0)
    shifted = scores - highest_each
    exponent = jnp.exp(shifted)
    totals = jnp.sum(jnp.where(member, exponent[None, :], 0.0), axis=1)
    weights = jnp.sum(jnp.where(member, relevance[None, :], 0.0), axis=1)
    total_each = jnp.sum(jnp.where(member, totals[:, None], 0.0), axis=0)
    weight_each = jnp.sum(jnp.where(member, weights[:, None], 0.0), axis=0)
    probability = exponent / total_each
    target = relevance / weight_each
    loss_sum = jnp.sum(jnp.log(totals)) - jnp.sum(target * shifted)
    return (loss_sum, probability - target)


def selector(indices, count):
    return (indices[:, None] == jnp.arange(count, dtype=jnp.int32)[None, :]).astype(jnp.bfloat16)


def pick_rows(indices, source):
    return jnp.dot(
        selector(indices, source.shape[0]), source, preferred_element_type=jnp.float32
    ).astype(jnp.bfloat16)


def place_rows(indices, values, count):
    return lax.dot_general(
        selector(indices, count),
        values,
        (((0,), (0,)), ((), ())),
        preferred_element_type=jnp.float32,
    )


def on_device(
    tables, owner_ids, row_ids, session_of, relevance, logit_bias, w_hidden, bias_hidden, w_score
):
    owners = lax.axis_size("table")
    devices = owners * lax.axis_size("dp")
    table_count, shard_rows, emb_width = tables.shape
    imp_count = row_ids.shape[2]
    capacity = 2 * imp_count // owners
    if (
        capacity % 16 == 0
        and table_count * capacity == 128
        and w_hidden.shape[0] == w_hidden.shape[1] == table_count * emb_width
        and emb_width == 128
    ):
        return whole_kernel(
            tables,
            owner_ids.reshape(table_count, 1, imp_count),
            row_ids[0],
            session_of,
            relevance,
            logit_bias,
            w_hidden,
            bias_hidden[None, :],
            w_score[None, :],
        )
    owner_now = owner_ids[0, :, :, 0]
    rows_now = row_ids[0]
    slot_total = owners * capacity
    one_hot = (owner_now[:, :, None] == jnp.arange(owners, dtype=jnp.int32)).astype(jnp.float32)
    places = jnp.arange(imp_count, dtype=jnp.int32)
    lower_tri = (places[:, None] >= places[None, :]).astype(jnp.float32)
    running = jnp.einsum("ij,tjo->tio", lower_tri, one_hot, precision=lax.Precision.HIGHEST)
    rank_in = (jnp.sum(running * one_hot, axis=2) - 1.0).astype(jnp.int32)
    slot_of = owner_now * capacity + rank_in
    slot_hot = (slot_of[:, :, None] == jnp.arange(slot_total, dtype=jnp.int32)).astype(jnp.int32)
    wanted = jnp.sum(slot_hot * rows_now[:, :, None], axis=1) + shard_rows * (
        1 - jnp.sum(slot_hot, axis=1)
    )
    requested = lax.all_to_all(
        wanted.reshape(table_count, owners, capacity),
        "table",
        split_axis=1,
        concat_axis=1,
        tiled=True,
    )
    served = lax.map(
        lambda pair: pick_rows(pair[0], pair[1]),
        (requested.reshape(table_count, slot_total), tables),
    )
    served = served.reshape(table_count, owners, capacity, emb_width)
    hidden_bf = w_hidden.astype(jnp.bfloat16)
    returned = lax.all_to_all(served, "table", split_axis=1, concat_axis=1, tiled=True).reshape(
        table_count, slot_total, emb_width
    )
    gathered = lax.map(lambda pair: pick_rows(pair[0], pair[1]), (slot_of, returned))
    inputs = jnp.transpose(gathered, (1, 0, 2)).reshape(imp_count, table_count * emb_width)
    pre_act = jnp.dot(inputs, hidden_bf, preferred_element_type=jnp.float32)
    pre_act = pre_act + bias_hidden
    hidden = jax.nn.silu(pre_act)
    scores = jnp.dot(hidden, w_score, precision=lax.Precision.HIGHEST) + logit_bias[0]
    loss_sum, score_grad = session_terms(scores, session_of[0], relevance[0], SESS_DEV)
    pre_grad = score_grad[:, None] * w_score[None, :] * silu_slope(pre_act)
    pre_grad_bf = pre_grad.astype(jnp.bfloat16)
    weight_grad = lax.dot_general(
        inputs, pre_grad_bf, (((0,), (0,)), ((), ())), preferred_element_type=jnp.float32
    )
    bias_grad = jnp.sum(pre_grad, axis=0)
    score_weight_grad = jnp.dot(score_grad, hidden, precision=lax.Precision.HIGHEST)
    input_grad = jnp.dot(pre_grad_bf, hidden_bf.T, preferred_element_type=jnp.float32).astype(
        jnp.bfloat16
    )
    input_grad = jnp.transpose(input_grad.reshape(imp_count, table_count, emb_width), (1, 0, 2))
    outgoing = lax.map(
        lambda pair: place_rows(pair[0], pair[1], slot_total).astype(jnp.bfloat16),
        (slot_of, input_grad),
    )
    incoming = lax.all_to_all(
        outgoing.reshape(table_count, owners, capacity, emb_width),
        "table",
        split_axis=1,
        concat_axis=1,
        tiled=True,
    )
    summed = lax.map(
        lambda pair: place_rows(pair[0], pair[1], shard_rows),
        (
            requested.reshape(table_count, slot_total),
            incoming.reshape(table_count, slot_total, emb_width),
        ),
    )
    own_rows = lax.psum_scatter(summed, "dp", scatter_dimension=1, tiled=True)
    emb_step = own_rows / (jnp.sqrt(jnp.mean(own_rows * own_rows, axis=2, keepdims=True)) + 1e-06)
    param_count = w_hidden.size + bias_hidden.size + w_score.size
    weight_tot, bias_tot, score_tot, loss_tot = lax.psum(
        (weight_grad, bias_grad, score_weight_grad, loss_sum), ("table", "dp")
    )
    mean_sq = (
        jnp.sum(weight_tot * weight_tot)
        + jnp.sum(bias_tot * bias_tot)
        + jnp.sum(score_tot * score_tot)
    ) / param_count
    factor = 1.0 / jnp.sqrt(mean_sq + 1e-06)
    step_hidden = weight_tot * factor
    loss = loss_tot / (SESS_DEV * devices)
    return (emb_step, step_hidden, bias_tot * factor, score_tot * factor, loss)


MESH = pl.DeviceIdType.MESH
F32, BF16, I16 = jnp.float32, jnp.bfloat16, jnp.int16
CHUNKS = 2
LANES = 128


def iota(shape, dim):
    return lax.broadcasted_iota(jnp.int32, shape, dim)


def ones_where(mask):
    return jnp.where(mask, 1.0, 0.0)


def lane_hits(key, base, blocks):
    at = [(iota((16, LANES), 1) + (base + k * LANES)).astype(I16) for k in range(blocks)]
    one, zero = jnp.ones(key.shape, BF16), jnp.zeros(key.shape, BF16)
    return jnp.concatenate(
        [
            jnp.where(key == jnp.concatenate([lanes] * (key.shape[0] // 16), axis=0), one, zero)
            for lanes in at
        ],
        axis=1,
    )


def whole_body(
    sizes, tables_hbm, owner_hbm, rows_hbm, session_hbm, relevance_hbm, place_hbm, weights_hbm,
    bias_hbm, scorer_hbm,
    emb_rows, share_q, share_s, small_ref,
    tables_ref, owner_ref, asked_rows, session_ref, relevance_ref, place_ref, weights_ref, bias_ref,
    scorer_ref, w_bf, meta_ref, columns_ref, want_ref, ids_in, ids_other, spread_ref, pack_ref,
    ids_cols, place_keys, high_ref, hot_ref, hot_rows, served, picked, gathered, inputs_t, out_ref,
    grads, swapped,
    dense_ref, from_other, sum_pair, plane_q, plane_s, from_plane_q, from_plane_s, sum_plane,
    column_q, column_s, from_column_q, from_column_s,
    extra_ref, extra_other, extra_plane, extra_column, extra_pair, extra_sum,
    load_sem, fetch_sem, want_sems, serve_send, serve_recv, ids_sems, grad_send,
    grad_recv, swap_send, swap_recv, pair_send, pair_recv, plane_send, plane_recv, column_send,
    column_recv, extra_send, extra_recv,
):
    tables, owners, capacity, width, half_rows, inner, outer, hid = sizes
    slots = owners * capacity
    imps = asked_rows.shape[1]
    shard_rows = 2 * half_rows
    me = lax.axis_index("table")
    core = lax.axis_index("dp")
    low, high = lax.rem(me, inner), me // inner
    other = (me, 1 - core)
    half = outer // 2

    barrier = pltpu.get_barrier_semaphore()

    def greet(step, carry):
        pl.semaphore_signal(
            barrier, inc=1, device_id=(lax.rem(me + step, owners), core), device_id_type=MESH
        )
        return carry

    pl.semaphore_signal(barrier, inc=1, device_id=other, device_id_type=MESH)
    lax.fori_loop(1, owners, greet, 0)

    sources = [
        (owner_hbm, owner_ref), (rows_hbm, asked_rows), (session_hbm, session_ref),
        (relevance_hbm, relevance_ref), (place_hbm, place_ref), (weights_hbm, weights_ref),
        (bias_hbm, bias_ref), (scorer_hbm, scorer_ref),
    ]
    fetches = [
        pltpu.make_async_copy(src, dst, fetch_sem.at[at]) for at, (src, dst) in enumerate(sources)
    ]

    def load(table):
        return pltpu.make_async_copy(
            tables_hbm.at[table], tables_ref.at[table], load_sem.at[table]
        )

    for fetch in fetches:
        fetch.start()
    for table in range(tables):
        load(table).start()

    def remote(src, dst, send, recv, to):
        return pltpu.make_async_remote_copy(
            src_ref=src, dst_ref=dst, send_sem=send, recv_sem=recv, device_id=to,
            device_id_type=MESH,
        )

    def to_peers(copy_to):
        def far(step, carry):
            plane = (1 - high // half) * half + step // inner
            copy_to(plane * inner + lax.rem(low + lax.rem(step, inner), inner)).start()
            return carry

        def near(step, carry):
            plane = (high // half) * half + lax.rem(lax.rem(high, half) + 1 + step // inner, half)
            copy_to(plane * inner + lax.rem(low + lax.rem(step, inner), inner)).start()
            return carry

        def level(step, carry):
            copy_to(high * inner + lax.rem(low + step, inner)).start()
            return carry

        lax.fori_loop(0, half * inner, far, 0)
        lax.fori_loop(0, (half - 1) * inner, near, 0)
        lax.fori_loop(1, inner, level, 0)

    for fetch in fetches[:5]:
        fetch.wait()
    asked = [ones_where(iota((owners, imps), 0) == owner_ref[table]) for table in range(tables)]
    upto = ones_where(iota((imps, imps), 0) <= iota((imps, imps), 1)).astype(BF16)
    running = jnp.dot(
        jnp.concatenate(asked, axis=0).astype(BF16), upto, preferred_element_type=F32
    )
    tops, lows, keys = [], [], []
    meta_ref[...] = jnp.zeros_like(meta_ref)
    for table in range(tables):
        rank = jnp.sum(
            asked[table] * running[table * owners : (table + 1) * owners], axis=0, keepdims=True
        ) - 1.0
        meta_ref[table : table + 1, :] = owner_ref[table].astype(F32) * capacity + rank
        code = asked_rows[table : table + 1, :] + 1
        tops.append(asked[table] * (code >> 6).astype(F32))
        lows.append(asked[table] * (code & 63).astype(F32))
        keys.append(
            ones_where(iota((LANES, imps), 0) == rank.astype(jnp.int32) + table * capacity)
        )
    codes = jnp.concatenate(
        [jnp.concatenate(tops, axis=1), jnp.concatenate(lows, axis=1)], axis=0
    ).astype(BF16)
    packed = lax.dot_general(
        codes, jnp.concatenate(keys, axis=1).astype(BF16), (((1,), (1,)), ((), ())),
        preferred_element_type=F32,
    )
    want_ref[...] = (packed[:owners] * 64.0 + packed[owners:]).reshape(owners, 1, LANES)
    with jax.named_scope("barrier_wait"):
        pl.semaphore_wait(barrier, owners)

    to_peers(
        lambda peer: remote(
            want_ref.at[peer], ids_in.at[me], want_sems.at[0], want_sems.at[1], (peer, core)
        )
    )
    ids_in[me] = want_ref[me]

    meta_ref[tables : tables + 1, :] = session_ref[...].astype(F32)
    meta_ref[tables + 1 : tables + 2, :] = relevance_ref[...]
    meta_ref[tables + 2 : tables + 3, :] = place_ref[...]
    columns_ref[...] = meta_ref[...].T
    block_of = lax.rem(iota((2 * LANES, tables * LANES), 0), LANES) // capacity
    scale = jnp.where(iota((2 * LANES, tables * LANES), 0) < LANES, 64.0, 1.0)
    spread_ref[...] = jnp.where(
        block_of == iota((2 * LANES, tables * LANES), 1) // LANES, scale, 0.0
    ).astype(BF16)
    pack_at = iota((8, 2 * LANES), 1)
    pack_ref[...] = jnp.where(
        lax.rem(pack_at, LANES) // capacity == iota((8, 2 * LANES), 0),
        jnp.where(pack_at < LANES, 64.0, 1.0), 0.0,
    ).astype(BF16)
    for fetch in fetches[5:]:
        fetch.wait()
    w_bf[...] = weights_ref[...].astype(BF16)

    def expand(ids):
        got = ids[...]
        top = jnp.floor(got * (1.0 / 64.0))
        shape = (owners, capacity, LANES)
        keep = lax.rem(iota(shape, 2), capacity) == iota(shape, 1)
        parts = [
            jnp.where(keep, jnp.broadcast_to(part, shape), 0.0).astype(BF16).reshape(slots, LANES)
            for part in (top, got - top * 64.0)
        ]
        return jnp.concatenate(parts, axis=1)

    def columns_of(codes):
        return jnp.dot(codes, spread_ref[...], preferred_element_type=F32)

    with jax.named_scope("ids_wait"):
        remote(
            want_ref.at[pl.ds(0, owners - 1)], ids_in.at[pl.ds(0, owners - 1)], want_sems.at[0],
            want_sems.at[1], other,
        ).wait()
    ids_copy = remote(ids_in, ids_other, ids_sems.at[0], ids_sems.at[1], other)
    ids_copy.start()
    codes_mine = expand(ids_in)
    ids_cols[...] = columns_of(codes_mine)

    def pick(table):
        code = ids_cols[:, table * LANES : (table + 1) * LANES]
        upper = code > half_rows
        key = jnp.where(upper, code - (half_rows + 1.0), code - 1.0).astype(jnp.int32).astype(I16)
        both = jnp.zeros((slots, 2 * width), F32)
        depth = 256
        for at in range(0, half_rows, depth):
            rows = jnp.concatenate(
                [
                    tables_ref[table, at : at + depth, :],
                    tables_ref[table, half_rows + at : half_rows + at + depth, :],
                ],
                axis=1,
            )
            both = both + jnp.dot(
                lane_hits(key, at, depth // LANES), rows, preferred_element_type=F32
            )
        served[table] = jnp.where(upper, both[:, width:], both[:, :width]).astype(BF16).reshape(
            owners, capacity, width
        )

    with jax.named_scope("pick"):
        for table in range(tables):
            load(table).wait()
            pick(table)
            picked[table, me] = served[table, me]
            to_peers(
                lambda peer, table=table: remote(
                    served.at[table, peer], picked.at[table, me], serve_send.at[table],
                    serve_recv.at[table], (peer, core),
                )
            )

    with jax.named_scope("prep"):
        for table in range(tables):
            hot_ref[table] = ones_where(
                iota((imps, slots), 1) == columns_ref[:, table : table + 1].astype(jnp.int32)
            ).astype(BF16)
            hot_rows[table] = ones_where(
                iota((slots, imps), 0) == meta_ref[table : table + 1, :].astype(jnp.int32)
            ).astype(BF16)
        quarter = half_rows // 2
        first = (core * half_rows).astype(F32)

        def place_prep(codes, columns, at):
            lanes = lax.dot_general(
                pack_ref[...], codes, (((1,), (1,)), ((), ())), preferred_element_type=F32
            ) - (first + 1.0)
            inside = (lanes >= 0.0) & (lanes < half_rows)
            key = jnp.where(lanes >= quarter, lanes - quarter, lanes)
            key = jnp.where(inside, key, -1.0).astype(jnp.int32)
            for table in range(tables):
                place_keys[table, :, at : at + slots] = jnp.broadcast_to(
                    key[table : table + 1, :], (16, slots)
                ).astype(I16)
                column = columns[:, table * LANES : (table + 1) * LANES]
                high_ref[table, at : at + slots, :] = ones_where(
                    column > first + quarter
                ).astype(BF16)

        place_prep(codes_mine, ids_cols[...], 0)
        ids_copy.wait()
        codes_theirs = expand(ids_other)
        place_prep(codes_theirs, columns_of(codes_theirs), slots)

    pre_act = jnp.broadcast_to(bias_ref[...], (imps, hid))
    for table in range(tables):
        with jax.named_scope(f"rows_wait{table}"):
            remote(
                served.at[table, pl.ds(0, owners - 1)], picked.at[table, pl.ds(0, owners - 1)],
                serve_send.at[table], serve_recv.at[table], other,
            ).wait()
        own = jnp.dot(
            hot_ref[table], picked[table].reshape(slots, width), preferred_element_type=F32
        )
        gathered[:, table * width : (table + 1) * width] = own.astype(BF16)
        inputs_t[table * width : (table + 1) * width, :] = own.T.astype(BF16)
    with jax.named_scope("dense"):
        pre_act = jnp.dot(gathered[...], w_bf[...], preferred_element_type=F32) + bias_ref[...]
        logistic = 1.0 / (1.0 + jnp.exp(-pre_act))
        hidden = pre_act * logistic
        session = columns_ref[:, tables : tables + 1].astype(jnp.int32)
        relevance = columns_ref[:, tables + 1 : tables + 2]
        scores = jnp.sum(hidden * scorer_ref[...], axis=1, keepdims=True)
        scores = scores + columns_ref[:, tables + 2 : tables + 3]
        member = iota((imps, LANES), 1) == session
        highest = jnp.max(jnp.where(member, scores, -jnp.inf), axis=0, keepdims=True)
        highest_each = jnp.sum(jnp.where(member, highest, 0.0), axis=1, keepdims=True)
        shifted = scores - highest_each
        exponent = jnp.exp(shifted)
        sums = jnp.sum(jnp.where(member, exponent, 0.0), axis=0, keepdims=True)
        weights = jnp.sum(jnp.where(member, relevance, 0.0), axis=0, keepdims=True)
        sum_each = jnp.sum(jnp.where(member, sums, 0.0), axis=1, keepdims=True)
        weight_each = jnp.sum(jnp.where(member, weights, 0.0), axis=1, keepdims=True)
        target = relevance / weight_each
        real = iota((1, LANES), 1) < SESS_DEV
        loss_sum = jnp.sum(jnp.log(jnp.where(real, sums, 1.0)), keepdims=True) - jnp.sum(
            target * shifted, keepdims=True
        )
        score_grad = exponent / sum_each - target
        pre_grad = score_grad * scorer_ref[...] * (logistic * (1.0 + pre_act * (1.0 - logistic)))
        pre_grad_bf = pre_grad.astype(BF16)
    piece, rows = hid // CHUNKS, hid // (2 * owners)

    def pair_up(chunk):
        return remote(
            dense_ref.at[chunk, 1 - core], from_other.at[chunk], pair_send.at[0, chunk],
            pair_recv.at[0, chunk], other,
        )

    with jax.named_scope("weight_grad"):
        for chunk in range(CHUNKS):
            dense_ref[chunk] = jnp.dot(
                inputs_t[...], pre_grad_bf[:, chunk * piece : (chunk + 1) * piece],
                preferred_element_type=F32,
            ).reshape(dense_ref.shape[1:])
            pair_up(chunk).start()
        extra_ref[...] = jnp.zeros_like(extra_ref)
        extra_ref[0:1, :] = jnp.sum(pre_grad, axis=0, keepdims=True)
        extra_ref[1:2, :] = jnp.sum(score_grad * hidden, axis=0, keepdims=True)
        extra_ref[2:3, :] = jnp.broadcast_to(loss_sum, (1, hid))
        extra_up = remote(extra_ref, extra_other, extra_send.at[0], extra_recv.at[0], other)
        extra_up.start()
    with jax.named_scope("input_grad"):
        input_grad = lax.dot_general(
            pre_grad_bf, w_bf[...], (((1,), (1,)), ((), ())), preferred_element_type=F32
        ).astype(BF16)

    def send_grads(table):
        out_ref[table] = jnp.dot(
            hot_rows[table], input_grad[:, table * width : (table + 1) * width],
            preferred_element_type=F32,
        ).astype(BF16).reshape(owners, capacity, width)
        grads[table, me] = out_ref[table, me]
        to_peers(
            lambda peer: remote(
                out_ref.at[table, peer], grads.at[table, me], grad_send.at[table],
                grad_recv.at[table], (peer, core),
            )
        )

    def swap(table):
        return remote(
            grads.at[table], swapped.at[table], swap_send.at[table], swap_recv.at[table], other
        )

    def arrive(table):
        remote(
            out_ref.at[table, pl.ds(0, owners - 1)], grads.at[table, pl.ds(0, owners - 1)],
            grad_send.at[table], grad_recv.at[table], other,
        ).wait()
        swap(table).start()

    def place(table):
        swap(table).wait()
        values = jnp.concatenate(
            [grads[table].reshape(slots, width), swapped[table].reshape(slots, width)], axis=0
        )
        upper = values * high_ref[table]
        values = jnp.concatenate([values - upper, upper], axis=1)
        block = 256
        one, zero = jnp.ones((block, LANES), BF16), jnp.zeros((block, LANES), BF16)
        for start in range(0, half_rows // 2, block):
            at = (iota((block, LANES), 0) + start).astype(I16)
            hits = [
                jnp.where(
                    jnp.concatenate(
                        [place_keys[table, :, lane : lane + LANES]] * (block // 16), axis=0
                    ) == at, one, zero,
                )
                for lane in range(0, 2 * slots, LANES)
            ]
            both = jnp.dot(jnp.concatenate(hits, axis=1), values, preferred_element_type=F32)
            for part in range(2):
                summed = both[:, part * width : (part + 1) * width]
                mean = jnp.sum(summed * summed, axis=1, keepdims=True) * (1.0 / width)
                rows_at = part * (half_rows // 2) + start
                emb_rows[table, rows_at : rows_at + block, :] = summed * (
                    1.0 / (jnp.sqrt(mean) + 1e-06)
                )

    def to_plane(src_of, dst_of, send, recv):
        for step in range(1, inner):
            to = lax.rem(low + step, inner)
            remote(src_of(to), dst_of(step - 1), send, recv, (high * inner + to, core)).start()

    def to_column(src_of, dst_of, send, recv):
        for step in range(1, outer):
            to = lax.rem(high + step, outer)
            remote(src_of(to), dst_of(step - 1), send, recv, (to * inner + low, core)).start()

    def await_all(src, dst, send, recv):
        remote(src, dst, send, recv, other).wait()

    def plane_sum(chunk):
        for at, (src, dst) in enumerate(((plane_s, from_plane_s), (plane_q, from_plane_q))):
            to_plane(
                lambda to: src.at[chunk, to], lambda slot: dst.at[chunk, slot],
                plane_send.at[at, chunk], plane_recv.at[at, chunk],
            )

    def plane_summed(chunk):
        for at, (src, dst) in enumerate(((plane_s, from_plane_s), (plane_q, from_plane_q))):
            await_all(
                src.at[chunk, pl.ds(0, inner - 1)], dst.at[chunk], plane_send.at[at, chunk],
                plane_recv.at[at, chunk],
            )

    def column_sum(chunk):
        for at, (src, dst) in enumerate(((column_s, from_column_s), (column_q, from_column_q))):
            to_column(
                lambda to: src.at[chunk, to], lambda slot: dst.at[chunk, slot],
                column_send.at[at, chunk], column_recv.at[at, chunk],
            )

    def column_summed(chunk):
        for at, (src, dst) in enumerate(((column_s, from_column_s), (column_q, from_column_q))):
            await_all(
                src.at[chunk, pl.ds(0, outer - 1)], dst.at[chunk], column_send.at[at, chunk],
                column_recv.at[at, chunk],
            )

    def column_share(chunk):
        for at, part in enumerate((share_s, share_q)):
            mine = part.at[chunk, core, low, high]
            to_column(
                lambda to: mine, lambda slot: mine, column_send.at[2 + at, chunk],
                column_recv.at[2 + at, chunk],
            )

    def column_shared(chunk):
        for at, part in enumerate((share_s, share_q)):
            some = part.at[chunk, core, low, pl.ds(0, outer - 1)]
            await_all(some, some, column_send.at[2 + at, chunk], column_recv.at[2 + at, chunk])

    def plane_share(chunk):
        for at, part in enumerate((share_s, share_q)):
            mine = part.at[chunk, core, low]
            to_plane(
                lambda to: mine, lambda slot: mine, plane_send.at[2 + at, chunk],
                plane_recv.at[2 + at, chunk],
            )

    def plane_shared(chunk):
        for at, part in enumerate((share_s, share_q)):
            some = part.at[chunk, core, pl.ds(0, inner - 1)]
            await_all(some, some, plane_send.at[2 + at, chunk], plane_recv.at[2 + at, chunk])

    def pair_down(chunk):
        return [
            remote(
                part.at[chunk, core], part.at[chunk, core], pair_send.at[phase, chunk],
                pair_recv.at[phase, chunk], other,
            )
            for phase, part in ((1, share_s), (2, share_q))
        ]

    def coded(values):
        most = jnp.max(jnp.abs(values), axis=0, keepdims=True)
        most = jnp.where(most < 1e-34, 0.0, most)
        code = jnp.round(values * jnp.where(most > 0.0, 32767.0 / most, 0.0))
        return code.astype(jnp.int32).astype(I16), most * (1.0 / 32767.0)

    def decoded(code, scale):
        return code.astype(jnp.int32).astype(F32) * scale

    def run(copies):
        for copy in copies:
            copy.start()

    def finish(copies):
        for copy in copies:
            copy.wait()

    def pair_step(chunk):
        pair_up(chunk).wait()
        for to in range(inner):
            values = dense_ref[chunk, core, to] + from_other[chunk, to]
            sum_pair[chunk, to] = values
            code, plane_s[chunk, to] = coded(values.reshape(outer * rows, piece))
            plane_q[chunk, to] = code.reshape(outer, rows, piece)
        plane_sum(chunk)
        if chunk == CHUNKS - 1:
            extra_up.wait()
            extra_pair[...] = extra_ref[...] + extra_other[...]
            extra_plane[low] = extra_ref[...] + extra_other[...]
            to_plane(
                lambda to: extra_pair, lambda slot: extra_plane.at[low], extra_send.at[1],
                extra_recv.at[1],
            )

    def plane_step(chunk):
        plane_summed(chunk)
        part = sum_pair[chunk, low].reshape(outer * rows, piece)
        for slot in range(inner - 1):
            part = part + decoded(
                from_plane_q[chunk, slot].reshape(outer * rows, piece), from_plane_s[chunk, slot]
            )
        for to in range(outer):
            values = part[to * rows : (to + 1) * rows]
            sum_plane[chunk, to] = values
            column_q[chunk, to], column_s[chunk, to] = coded(values)
        column_sum(chunk)
        if chunk == CHUNKS - 1:
            some = extra_plane.at[pl.ds(0, inner - 1)]
            await_all(some, some, extra_send.at[1], extra_recv.at[1])
            part = extra_plane[0]
            for slot in range(1, inner):
                part = part + extra_plane[slot]
            extra_sum[...] = part
            extra_column[high] = part
            to_column(
                lambda to: extra_sum, lambda slot: extra_column.at[high], extra_send.at[2],
                extra_recv.at[2],
            )

    def column_step(chunk):
        column_summed(chunk)
        part = sum_plane[chunk, high]
        for slot in range(outer - 1):
            part = part + decoded(from_column_q[chunk, slot], from_column_s[chunk, slot])
        code, scale = coded(part)
        share_q[chunk, core, low, high] = code
        share_s[chunk, core, low, high] = scale
        column_share(chunk)
        if chunk == CHUNKS - 1:
            some = extra_column.at[pl.ds(0, outer - 1)]
            await_all(some, some, extra_send.at[2], extra_recv.at[2])
            part = extra_column[0]
            for slot in range(1, outer):
                part = part + extra_column[slot]
            small_ref[...] = part

    def share_step(chunk):
        column_shared(chunk)
        plane_share(chunk)

    def down_step(chunk):
        plane_shared(chunk)
        run(pair_down(chunk))

    def last_step(chunk):
        finish(pair_down(chunk))

    steps = {
        "send": send_grads, "pair": pair_step, "plane": plane_step, "column": column_step,
        "share": share_step, "down": down_step, "last": last_step, "arrive": arrive, "place": place,
    }
    for word in ORDER:
        with jax.named_scope(word):
            steps[word[:-1]](int(word[-1]))


ORDER = (
    "send0", "pair0", "pair1", "send1", "send2", "plane0", "send3", "plane1", "arrive0",
    "place0", "column0", "arrive1", "place1", "column1", "arrive2", "share0", "share1",
    "place2", "arrive3", "down0", "down1", "place3", "last0", "last1",
)


def write_body(
    params, sessions, rows_hbm, code_ref, scale_ref, small_ref, emb_hbm, hidden_hbm, bias_hbm,
    score_hbm, loss_hbm, hidden_ref, bias_ref, score_ref, loss_ref, row_sems, sems,
):
    copies = [
        pltpu.make_async_copy(rows_hbm.at[table], emb_hbm.at[table], row_sems.at[table])
        for table in range(rows_hbm.shape[0])
    ]
    for copy in copies:
        copy.start()
    hid = hidden_ref.shape[0]
    piece = code_ref.shape[-1]
    small = small_ref[...]
    counts = jnp.where(iota(small.shape, 0) < 2, small, 0.0)
    squares = jnp.sum(counts * counts, keepdims=True)
    for chunk in range(hid // piece):
        part = code_ref[chunk].astype(jnp.int32).astype(F32) * scale_ref[chunk]
        part = part.reshape(hid, piece)
        hidden_ref[:, chunk * piece : (chunk + 1) * piece] = part
        squares = squares + jnp.sum(part * part, keepdims=True)
    factor = 1.0 / jnp.sqrt(squares / params + 1e-06)
    hidden_ref[...] = hidden_ref[...] * factor
    bias_ref[...] = small[0:1, :] * factor
    score_ref[...] = small[1:2, :] * factor
    loss_ref[...] = small[2:3, 0:1] / sessions
    for at, (src, dst) in enumerate(
        (
            (hidden_ref, hidden_hbm), (bias_ref, bias_hbm), (score_ref, score_hbm),
            (loss_ref, loss_hbm),
        )
    ):
        copies.append(pltpu.make_async_copy(src, dst, sems.at[at]))
        copies[-1].start()
    for copy in copies:
        copy.wait()


def whole_kernel(
    tables, owner_ids, row_ids, session, relevance, logit_bias, w_hidden, bias_hidden, w_score
):
    table_count, shard_rows, width = tables.shape
    owners = lax.axis_size("table")
    imps = row_ids.shape[1]
    capacity = 2 * imps // owners
    hid = w_hidden.shape[1]
    slots = owners * capacity
    half_rows = shard_rows // 2
    inner = 1
    while inner * inner < owners:
        inner *= 2
    outer = owners // inner
    rows = hid // (2 * owners)
    piece = hid // CHUNKS
    sizes = (table_count, owners, capacity, width, half_rows, inner, outer, hid)
    dma = pltpu.SemaphoreType.DMA
    vmem = pl.BlockSpec(memory_space=pltpu.VMEM)
    hbm = pl.BlockSpec(memory_space=pltpu.HBM)
    lookups = (table_count, owners, capacity, width)
    emb_rows, codes, scales, small = pl.pallas_call(
        functools.partial(whole_body, sizes),
        out_shape=(
            jax.ShapeDtypeStruct((table_count, half_rows, width), F32),
            jax.ShapeDtypeStruct((CHUNKS, 2, inner, outer, rows, piece), I16),
            jax.ShapeDtypeStruct((CHUNKS, 2, inner, outer, 1, piece), F32),
            jax.ShapeDtypeStruct((8, hid), F32),
        ),
        in_specs=[hbm] * 9,
        out_specs=(vmem, vmem, vmem, vmem),
        scratch_shapes=[
            pltpu.VMEM(tables.shape, BF16),
            pltpu.VMEM(owner_ids.shape, jnp.int32),
            pltpu.VMEM(row_ids.shape, jnp.int32),
            pltpu.VMEM(session.shape, jnp.int32),
            pltpu.VMEM(relevance.shape, F32),
            pltpu.VMEM(logit_bias.shape, F32),
            pltpu.VMEM(w_hidden.shape, F32),
            pltpu.VMEM(bias_hidden.shape, F32),
            pltpu.VMEM(w_score.shape, F32),
            pltpu.VMEM(w_hidden.shape, BF16),
            pltpu.VMEM((LANES, imps), F32),
            pltpu.VMEM((imps, LANES), F32),
            pltpu.VMEM((owners, 1, LANES), F32),
            pltpu.VMEM((owners, 1, LANES), F32),
            pltpu.VMEM((owners, 1, LANES), F32),
            pltpu.VMEM((2 * LANES, table_count * LANES), BF16),
            pltpu.VMEM((8, 2 * LANES), BF16),
            pltpu.VMEM((slots, table_count * LANES), F32),
            pltpu.VMEM((table_count, 16, 2 * slots), I16),
            pltpu.VMEM((table_count, 2 * slots, LANES), BF16),
            pltpu.VMEM((table_count, imps, slots), BF16),
            pltpu.VMEM((table_count, slots, imps), BF16),
            pltpu.VMEM(lookups, BF16),
            pltpu.VMEM(lookups, BF16),
            pltpu.VMEM((imps, table_count * width), BF16),
            pltpu.VMEM((table_count * width, imps), BF16),
            pltpu.VMEM(lookups, BF16),
            pltpu.VMEM(lookups, BF16),
            pltpu.VMEM(lookups, BF16),
            pltpu.VMEM((CHUNKS, 2, inner, outer, rows, piece), F32),
            pltpu.VMEM((CHUNKS, inner, outer, rows, piece), F32),
            pltpu.VMEM((CHUNKS, inner, outer, rows, piece), F32),
            pltpu.VMEM((CHUNKS, inner, outer, rows, piece), I16),
            pltpu.VMEM((CHUNKS, inner, 1, piece), F32),
            pltpu.VMEM((CHUNKS, inner - 1, outer, rows, piece), I16),
            pltpu.VMEM((CHUNKS, inner - 1, 1, piece), F32),
            pltpu.VMEM((CHUNKS, outer, rows, piece), F32),
            pltpu.VMEM((CHUNKS, outer, rows, piece), I16),
            pltpu.VMEM((CHUNKS, outer, 1, piece), F32),
            pltpu.VMEM((CHUNKS, outer - 1, rows, piece), I16),
            pltpu.VMEM((CHUNKS, outer - 1, 1, piece), F32),
            pltpu.VMEM((8, hid), F32),
            pltpu.VMEM((8, hid), F32),
            pltpu.VMEM((inner, 8, hid), F32),
            pltpu.VMEM((outer, 8, hid), F32),
            pltpu.VMEM((8, hid), F32),
            pltpu.VMEM((8, hid), F32),
            dma((table_count,)), dma((8,)), dma((2,)),
            dma((table_count,)), dma((table_count,)), dma((2,)), dma((table_count,)),
            dma((table_count,)), dma((table_count,)), dma((table_count,)),
            dma((3, CHUNKS)), dma((3, CHUNKS)),
            dma((4, CHUNKS)), dma((4, CHUNKS)), dma((4, CHUNKS)), dma((4, CHUNKS)),
            dma((3,)), dma((3,)),
        ],
        compiler_params=pltpu.CompilerParams(
            collective_id=1, has_side_effects=True, vmem_limit_bytes=44 * 1024 * 1024
        ),
    )(
        *(
            pltpu.with_memory_space_constraint(operand, pltpu.HBM)
            for operand in (
                tables, owner_ids, row_ids, session, relevance, logit_bias, w_hidden, bias_hidden,
                w_score,
            )
        )
    )
    params = hid * hid + 2 * hid
    emb_step, step_hidden, step_bias, step_score, loss = pl.pallas_call(
        functools.partial(write_body, params, SESS_DEV * owners * 2),
        out_shape=(
            jax.ShapeDtypeStruct((table_count, half_rows, width), F32),
            jax.ShapeDtypeStruct((hid, hid), F32),
            jax.ShapeDtypeStruct((1, hid), F32),
            jax.ShapeDtypeStruct((1, hid), F32),
            jax.ShapeDtypeStruct((1, 1), F32),
        ),
        in_specs=[vmem] * 4,
        out_specs=(hbm,) * 5,
        scratch_shapes=[
            pltpu.VMEM((hid, hid), F32), pltpu.VMEM((1, hid), F32), pltpu.VMEM((1, hid), F32),
            pltpu.VMEM((1, 1), F32), dma((table_count,)), dma((4,)),
        ],
        compiler_params=pltpu.CompilerParams(vmem_limit_bytes=8 * 1024 * 1024),
    )(emb_rows, codes, scales, small)
    return (emb_step, step_hidden, step_bias[0], step_score[0], loss[0, 0])


def solution(mesh):
    in_specs = (
        P(None, "table", None),
        P(("table", "dp"), None, None, None),
        P(("table", "dp"), None, None),
        P(("table", "dp"), None),
        P(("table", "dp"), None),
        P(("table", "dp"), None),
        P(),
        P(),
        P(),
    )
    out_specs = (P(None, ("table", "dp"), None), P(), P(), P(), P())
    return jax.shard_map(
        on_device, mesh=mesh, in_specs=in_specs, out_specs=out_specs, check_vma=False
    )
```

```python
import jax
import jax.numpy as jnp
from jax import lax
from jax.experimental import pallas as pl
from jax.experimental.pallas import tpu as pltpu
import functools
from jax.sharding import PartitionSpec as P

SESS_DEV = 2


def silu_slope(pre_val):
    logistic = jax.nn.sigmoid(pre_val)
    return logistic * (1.0 + pre_val * (1.0 - logistic))


def session_terms(scores, session_ids, relevance, sessions):
    member = session_ids[None, :] == jnp.arange(sessions, dtype=jnp.int32)[:, None]
    highest = jnp.max(jnp.where(member, scores[None, :], -jnp.inf), axis=1)
    highest_each = jnp.sum(jnp.where(member, highest[:, None], 0.0), axis=0)
    shifted = scores - highest_each
    exponent = jnp.exp(shifted)
    totals = jnp.sum(jnp.where(member, exponent[None, :], 0.0), axis=1)
    weights = jnp.sum(jnp.where(member, relevance[None, :], 0.0), axis=1)
    total_each = jnp.sum(jnp.where(member, totals[:, None], 0.0), axis=0)
    weight_each = jnp.sum(jnp.where(member, weights[:, None], 0.0), axis=0)
    probability = exponent / total_each
    target = relevance / weight_each
    loss_sum = jnp.sum(jnp.log(totals)) - jnp.sum(target * shifted)
    return (loss_sum, probability - target)


def selector(indices, count):
    return (indices[:, None] == jnp.arange(count, dtype=jnp.int32)[None, :]).astype(jnp.bfloat16)


def pick_rows(indices, source):
    return jnp.dot(
        selector(indices, source.shape[0]), source, preferred_element_type=jnp.float32
    ).astype(jnp.bfloat16)


def place_rows(indices, values, count):
    return lax.dot_general(
        selector(indices, count),
        values,
        (((0,), (0,)), ((), ())),
        preferred_element_type=jnp.float32,
    )


def on_device(
    tables, owner_ids, row_ids, session_of, relevance, logit_bias, w_hidden, bias_hidden, w_score
):
    owners = lax.axis_size("table")
    devices = owners * lax.axis_size("dp")
    table_count, shard_rows, emb_width = tables.shape
    imp_count = row_ids.shape[2]
    capacity = 2 * imp_count // owners
    if (
        capacity % 16 == 0
        and table_count * capacity == 128
        and w_hidden.shape[0] == w_hidden.shape[1] == table_count * emb_width
        and emb_width == 128
    ):
        return whole_kernel(
            tables,
            owner_ids.reshape(table_count, 1, imp_count),
            row_ids[0],
            session_of,
            relevance,
            logit_bias,
            w_hidden,
            bias_hidden[None, :],
            w_score[None, :],
        )
    owner_now = owner_ids[0, :, :, 0]
    rows_now = row_ids[0]
    slot_total = owners * capacity
    one_hot = (owner_now[:, :, None] == jnp.arange(owners, dtype=jnp.int32)).astype(jnp.float32)
    places = jnp.arange(imp_count, dtype=jnp.int32)
    lower_tri = (places[:, None] >= places[None, :]).astype(jnp.float32)
    running = jnp.einsum("ij,tjo->tio", lower_tri, one_hot, precision=lax.Precision.HIGHEST)
    rank_in = (jnp.sum(running * one_hot, axis=2) - 1.0).astype(jnp.int32)
    slot_of = owner_now * capacity + rank_in
    slot_hot = (slot_of[:, :, None] == jnp.arange(slot_total, dtype=jnp.int32)).astype(jnp.int32)
    wanted = jnp.sum(slot_hot * rows_now[:, :, None], axis=1) + shard_rows * (
        1 - jnp.sum(slot_hot, axis=1)
    )
    requested = lax.all_to_all(
        wanted.reshape(table_count, owners, capacity),
        "table",
        split_axis=1,
        concat_axis=1,
        tiled=True,
    )
    served = lax.map(
        lambda pair: pick_rows(pair[0], pair[1]),
        (requested.reshape(table_count, slot_total), tables),
    )
    served = served.reshape(table_count, owners, capacity, emb_width)
    hidden_bf = w_hidden.astype(jnp.bfloat16)
    returned = lax.all_to_all(served, "table", split_axis=1, concat_axis=1, tiled=True).reshape(
        table_count, slot_total, emb_width
    )
    gathered = lax.map(lambda pair: pick_rows(pair[0], pair[1]), (slot_of, returned))
    inputs = jnp.transpose(gathered, (1, 0, 2)).reshape(imp_count, table_count * emb_width)
    pre_act = jnp.dot(inputs, hidden_bf, preferred_element_type=jnp.float32)
    pre_act = pre_act + bias_hidden
    hidden = jax.nn.silu(pre_act)
    scores = jnp.dot(hidden, w_score, precision=lax.Precision.HIGHEST) + logit_bias[0]
    loss_sum, score_grad = session_terms(scores, session_of[0], relevance[0], SESS_DEV)
    pre_grad = score_grad[:, None] * w_score[None, :] * silu_slope(pre_act)
    pre_grad_bf = pre_grad.astype(jnp.bfloat16)
    weight_grad = lax.dot_general(
        inputs, pre_grad_bf, (((0,), (0,)), ((), ())), preferred_element_type=jnp.float32
    )
    bias_grad = jnp.sum(pre_grad, axis=0)
    score_weight_grad = jnp.dot(score_grad, hidden, precision=lax.Precision.HIGHEST)
    input_grad = jnp.dot(pre_grad_bf, hidden_bf.T, preferred_element_type=jnp.float32).astype(
        jnp.bfloat16
    )
    input_grad = jnp.transpose(input_grad.reshape(imp_count, table_count, emb_width), (1, 0, 2))
    outgoing = lax.map(
        lambda pair: place_rows(pair[0], pair[1], slot_total).astype(jnp.bfloat16),
        (slot_of, input_grad),
    )
    incoming = lax.all_to_all(
        outgoing.reshape(table_count, owners, capacity, emb_width),
        "table",
        split_axis=1,
        concat_axis=1,
        tiled=True,
    )
    summed = lax.map(
        lambda pair: place_rows(pair[0], pair[1], shard_rows),
        (
            requested.reshape(table_count, slot_total),
            incoming.reshape(table_count, slot_total, emb_width),
        ),
    )
    own_rows = lax.psum_scatter(summed, "dp", scatter_dimension=1, tiled=True)
    emb_step = own_rows / (jnp.sqrt(jnp.mean(own_rows * own_rows, axis=2, keepdims=True)) + 1e-06)
    param_count = w_hidden.size + bias_hidden.size + w_score.size
    weight_tot, bias_tot, score_tot, loss_tot = lax.psum(
        (weight_grad, bias_grad, score_weight_grad, loss_sum), ("table", "dp")
    )
    mean_sq = (
        jnp.sum(weight_tot * weight_tot)
        + jnp.sum(bias_tot * bias_tot)
        + jnp.sum(score_tot * score_tot)
    ) / param_count
    factor = 1.0 / jnp.sqrt(mean_sq + 1e-06)
    step_hidden = weight_tot * factor
    loss = loss_tot / (SESS_DEV * devices)
    return (emb_step, step_hidden, bias_tot * factor, score_tot * factor, loss)


MESH = pl.DeviceIdType.MESH
F32, BF16, I16 = jnp.float32, jnp.bfloat16, jnp.int16
CHUNKS = 2
LANES = 128


def iota(shape, dim):
    return lax.broadcasted_iota(jnp.int32, shape, dim)


def ones_where(mask):
    return jnp.where(mask, 1.0, 0.0)


def lane_hits(key, base, blocks):
    at = [(iota((16, LANES), 1) + (base + k * LANES)).astype(I16) for k in range(blocks)]
    one, zero = jnp.ones(key.shape, BF16), jnp.zeros(key.shape, BF16)
    return jnp.concatenate(
        [
            jnp.where(key == jnp.concatenate([lanes] * (key.shape[0] // 16), axis=0), one, zero)
            for lanes in at
        ],
        axis=1,
    )


def whole_body(
    sizes, tables_hbm, owner_hbm, rows_hbm, session_hbm, relevance_hbm, place_hbm, weights_hbm,
    bias_hbm, scorer_hbm,
    emb_rows, share_q, share_s, small_ref,
    tables_ref, owner_ref, asked_rows, session_ref, relevance_ref, place_ref, weights_ref, bias_ref,
    scorer_ref, w_bf, meta_ref, columns_ref, want_ref, ids_in, ids_other, spread_ref, pack_ref,
    ids_cols, place_keys, high_ref, hot_ref, hot_rows, served, picked, gathered, inputs_t, out_ref,
    grads, swapped,
    dense_ref, from_other, sum_pair, plane_q, plane_s, from_plane_q, from_plane_s, sum_plane,
    column_q, column_s, from_column_q, from_column_s,
    extra_ref, extra_other, extra_plane, extra_column, extra_pair, extra_sum,
    load_sem, fetch_sem, want_sems, serve_send, serve_recv, ids_sems, grad_send,
    grad_recv, swap_send, swap_recv, pair_send, pair_recv, plane_send, plane_recv, column_send,
    column_recv, extra_send, extra_recv,
):
    tables, owners, capacity, width, half_rows, inner, outer, hid = sizes
    slots = owners * capacity
    imps = asked_rows.shape[1]
    shard_rows = 2 * half_rows
    me = lax.axis_index("table")
    core = lax.axis_index("dp")
    low, high = lax.rem(me, inner), me // inner
    other = (me, 1 - core)
    half = outer // 2
    is_hub = (high >= half - 1) & (high <= half)

    barrier = pltpu.get_barrier_semaphore()

    def greet(step, carry):
        pl.semaphore_signal(
            barrier, inc=1, device_id=(lax.rem(me + step, owners), core), device_id_type=MESH
        )
        return carry

    pl.semaphore_signal(barrier, inc=1, device_id=other, device_id_type=MESH)
    lax.fori_loop(1, owners, greet, 0)

    sources = [
        (owner_hbm, owner_ref), (rows_hbm, asked_rows), (session_hbm, session_ref),
        (relevance_hbm, relevance_ref), (place_hbm, place_ref), (weights_hbm, weights_ref),
        (bias_hbm, bias_ref), (scorer_hbm, scorer_ref),
    ]
    fetches = [
        pltpu.make_async_copy(src, dst, fetch_sem.at[at]) for at, (src, dst) in enumerate(sources)
    ]

    load = pltpu.make_async_copy(tables_hbm, tables_ref, load_sem.at[0])

    for fetch in fetches:
        fetch.start()
    load.start()

    def remote(src, dst, send, recv, to):
        return pltpu.make_async_remote_copy(
            src_ref=src, dst_ref=dst, send_sem=send, recv_sem=recv, device_id=to,
            device_id_type=MESH,
        )

    def to_peers(copy_to, far_too=True, near_too=True):
        def far(step, carry):
            plane = (1 - high // half) * half + step // inner
            copy_to(plane * inner + lax.rem(low + lax.rem(step, inner), inner)).start()
            return carry

        def near(step, carry):
            plane = (high // half) * half + lax.rem(lax.rem(high, half) + 1 + step // inner, half)
            copy_to(plane * inner + lax.rem(low + lax.rem(step, inner), inner)).start()
            return carry

        def level(step, carry):
            copy_to(high * inner + lax.rem(low + step, inner)).start()
            return carry

        if far_too:
            lax.fori_loop(0, half * inner, far, 0)
        if near_too:
            lax.fori_loop(0, (half - 1) * inner, near, 0)
            lax.fori_loop(1, inner, level, 0)

    for fetch in fetches[:5]:
        fetch.wait()
    asked = [ones_where(iota((owners, imps), 0) == owner_ref[table]) for table in range(tables)]
    upto = ones_where(iota((imps, imps), 0) <= iota((imps, imps), 1)).astype(BF16)
    running = jnp.dot(
        jnp.concatenate(asked, axis=0).astype(BF16), upto, preferred_element_type=F32
    )
    tops, lows, keys = [], [], []
    meta_ref[...] = jnp.zeros_like(meta_ref)
    for table in range(tables):
        rank = jnp.sum(
            asked[table] * running[table * owners : (table + 1) * owners], axis=0, keepdims=True
        ) - 1.0
        meta_ref[table : table + 1, :] = owner_ref[table].astype(F32) * capacity + rank
        code = asked_rows[table : table + 1, :] + 1
        tops.append(asked[table] * (code >> 6).astype(F32))
        lows.append(asked[table] * (code & 63).astype(F32))
        keys.append(
            ones_where(iota((LANES, imps), 0) == rank.astype(jnp.int32) + table * capacity)
        )
    codes = jnp.concatenate(
        [jnp.concatenate(tops, axis=1), jnp.concatenate(lows, axis=1)], axis=0
    ).astype(BF16)
    packed = lax.dot_general(
        codes, jnp.concatenate(keys, axis=1).astype(BF16), (((1,), (1,)), ((), ())),
        preferred_element_type=F32,
    )
    want_ref[...] = (packed[:owners] * 64.0 + packed[owners:]).reshape(owners, 1, LANES)
    with jax.named_scope("barrier_wait"):
        pl.semaphore_wait(barrier, owners)

    to_peers(
        lambda peer: remote(
            want_ref.at[peer], ids_in.at[me], want_sems.at[0], want_sems.at[1], (peer, core)
        )
    )
    ids_in[me] = want_ref[me]

    meta_ref[tables : tables + 1, :] = session_ref[...].astype(F32)
    meta_ref[tables + 1 : tables + 2, :] = relevance_ref[...]
    meta_ref[tables + 2 : tables + 3, :] = place_ref[...]
    columns_ref[...] = meta_ref[...].T
    block_of = lax.rem(iota((2 * LANES, tables * LANES), 0), LANES) // capacity
    scale = jnp.where(iota((2 * LANES, tables * LANES), 0) < LANES, 64.0, 1.0)
    spread_ref[...] = jnp.where(
        block_of == iota((2 * LANES, tables * LANES), 1) // LANES, scale, 0.0
    ).astype(BF16)
    pack_at = iota((8, 2 * LANES), 1)
    pack_ref[...] = jnp.where(
        lax.rem(pack_at, LANES) // capacity == iota((8, 2 * LANES), 0),
        jnp.where(pack_at < LANES, 64.0, 1.0), 0.0,
    ).astype(BF16)
    for fetch in fetches[5:]:
        fetch.wait()
    w_bf[...] = weights_ref[...].astype(BF16)

    def expand(ids):
        got = ids[...]
        top = jnp.floor(got * (1.0 / 64.0))
        shape = (owners, capacity, LANES)
        keep = lax.rem(iota(shape, 2), capacity) == iota(shape, 1)
        parts = [
            jnp.where(keep, jnp.broadcast_to(part, shape), 0.0).astype(BF16).reshape(slots, LANES)
            for part in (top, got - top * 64.0)
        ]
        return jnp.concatenate(parts, axis=1)

    def columns_of(codes):
        return jnp.dot(codes, spread_ref[...], preferred_element_type=F32)

    with jax.named_scope("ids_wait"):
        remote(
            want_ref.at[pl.ds(0, owners - 1)], ids_in.at[pl.ds(0, owners - 1)], want_sems.at[0],
            want_sems.at[1], other,
        ).wait()
    ids_copy = remote(ids_in, ids_other, ids_sems.at[0], ids_sems.at[1], other)
    ids_copy.start()
    codes_mine = expand(ids_in)
    ids_cols[...] = columns_of(codes_mine)

    def pick(table, first, count):
        code = ids_cols[
            pl.ds(pl.multiple_of(first * capacity, capacity), count * capacity),
            table * LANES : (table + 1) * LANES,
        ]
        upper = code > half_rows
        key = jnp.where(upper, code - (half_rows + 1.0), code - 1.0).astype(jnp.int32).astype(I16)
        both = jnp.zeros((count * capacity, 2 * width), F32)
        depth = 256
        for at in range(0, half_rows, depth):
            rows = jnp.concatenate(
                [
                    tables_ref[table, at : at + depth, :],
                    tables_ref[table, half_rows + at : half_rows + at + depth, :],
                ],
                axis=1,
            )
            both = both + jnp.dot(
                lane_hits(key, at, depth // LANES), rows, preferred_element_type=F32
            )
        served[table, pl.ds(first, count)] = (
            jnp.where(upper, both[:, width:], both[:, :width])
            .astype(BF16)
            .reshape(count, capacity, width)
        )

    def serve(table, far_too, near_too):
        to_peers(
            lambda peer: remote(
                served.at[table, peer], picked.at[table, me], serve_send.at[table],
                serve_recv.at[table], (peer, core),
            ),
            far_too, near_too,
        )

    with jax.named_scope("pick"):
        load.wait()
        side = high // half
        part = owners // 2
        pick(0, (1 - side) * part, part)
        serve(0, True, False)
        pick(0, side * part, part)
        serve(0, False, True)
        for table in range(1, tables):
            pick(table, 0, owners)
            serve(table, True, True)
        for table in range(tables):
            picked[table, me] = served[table, me]

    with jax.named_scope("prep"):
        for table in range(tables):
            hot_ref[table] = ones_where(
                iota((imps, slots), 1) == columns_ref[:, table : table + 1].astype(jnp.int32)
            ).astype(BF16)
            hot_rows[table] = ones_where(
                iota((slots, imps), 0) == meta_ref[table : table + 1, :].astype(jnp.int32)
            ).astype(BF16)
        quarter = half_rows // 2
        first = (core * half_rows).astype(F32)

        def place_prep(codes, columns, at):
            lanes = lax.dot_general(
                pack_ref[...], codes, (((1,), (1,)), ((), ())), preferred_element_type=F32
            ) - (first + 1.0)
            inside = (lanes >= 0.0) & (lanes < half_rows)
            key = jnp.where(lanes >= quarter, lanes - quarter, lanes)
            key = jnp.where(inside, key, -1.0).astype(jnp.int32)
            for table in range(tables):
                place_keys[table, :, at : at + slots] = jnp.broadcast_to(
                    key[table : table + 1, :], (16, slots)
                ).astype(I16)
                column = columns[:, table * LANES : (table + 1) * LANES]
                high_ref[table, at : at + slots, :] = ones_where(
                    column > first + quarter
                ).astype(BF16)

        place_prep(codes_mine, ids_cols[...], 0)
        ids_copy.wait()
        codes_theirs = expand(ids_other)
        place_prep(codes_theirs, columns_of(codes_theirs), slots)

    session = columns_ref[:, tables : tables + 1].astype(jnp.int32)
    relevance = columns_ref[:, tables + 1 : tables + 2]

    def of_session(values, reduce, fill):
        found = [
            reduce(jnp.where(session == at, values, fill), axis=0, keepdims=True)
            for at in range(SESS_DEV)
        ]
        each = jnp.broadcast_to(found[-1], values.shape)
        for at in range(SESS_DEV - 1):
            each = jnp.where(session == at, found[at], each)
        return found, each

    target = relevance / of_session(relevance, jnp.sum, 0.0)[1]
    for table in range(tables):
        with jax.named_scope(f"rows_wait{table}"):
            remote(
                served.at[table, pl.ds(0, owners - 1)], picked.at[table, pl.ds(0, owners - 1)],
                serve_send.at[table], serve_recv.at[table], other,
            ).wait()
        own = jnp.dot(
            hot_ref[table], picked[table].reshape(slots, width), preferred_element_type=F32
        )
        gathered[:, table * width : (table + 1) * width] = own.astype(BF16)
        inputs_t[table * width : (table + 1) * width, :] = own.T.astype(BF16)
    with jax.named_scope("dense"):
        pre_act = jnp.dot(gathered[...], w_bf[...], preferred_element_type=F32) + bias_ref[...]
        logistic = 1.0 / (1.0 + jnp.exp(-pre_act))
        hidden = pre_act * logistic
        scores = jnp.sum(hidden * scorer_ref[...], axis=1, keepdims=True)
        scores = scores + columns_ref[:, tables + 2 : tables + 3]
        shifted = scores - of_session(scores, jnp.max, -jnp.inf)[1]
        exponent = jnp.exp(shifted)
        sums, sum_each = of_session(exponent, jnp.sum, 0.0)
        loss_sum = sum(jnp.log(value) for value in sums) - jnp.sum(target * shifted, keepdims=True)
        score_grad = exponent / sum_each - target
        pre_grad = score_grad * scorer_ref[...] * (logistic * (1.0 + pre_act * (1.0 - logistic)))
        pre_grad_bf = pre_grad.astype(BF16)
    piece, rows = hid // CHUNKS, hid // (4 * inner)

    def pair_up(chunk):
        return remote(
            dense_ref.at[chunk, 1 - core], from_other.at[chunk], pair_send.at[0, chunk],
            pair_recv.at[0, chunk], other,
        )

    extra_up = remote(extra_ref, extra_other, extra_send.at[0], extra_recv.at[0], other)

    def weight_step(chunk):
        dense_ref[chunk] = jnp.dot(
            inputs_t[...], pre_grad_bf[:, chunk * piece : (chunk + 1) * piece],
            preferred_element_type=F32,
        ).reshape(dense_ref.shape[1:])
        pair_up(chunk).start()
        if chunk == CHUNKS - 1:
            extra_ref[...] = jnp.zeros_like(extra_ref)
            extra_ref[0:1, :] = jnp.sum(pre_grad, axis=0, keepdims=True)
            extra_ref[1:2, :] = jnp.sum(score_grad * hidden, axis=0, keepdims=True)
            extra_ref[2:3, :] = jnp.broadcast_to(loss_sum, (1, hid))
            extra_up.start()

    def give(table, far_too, near_too):
        to_peers(
            lambda peer: remote(
                out_ref.at[table, peer], grads.at[table, me], grad_send.at[table],
                grad_recv.at[table], (peer, core),
            ),
            far_too, near_too,
        )

    def near_step(table):
        give(table, False, True)

    def send_grads(table):
        input_grad = lax.dot_general(
            pre_grad_bf, w_bf[table * width : (table + 1) * width, :], (((1,), (1,)), ((), ())),
            preferred_element_type=F32,
        ).astype(BF16)
        out_ref[table] = jnp.dot(
            hot_rows[table], input_grad, preferred_element_type=F32
        ).astype(BF16).reshape(owners, capacity, width)
        grads[table, me] = out_ref[table, me]
        give(table, True, False)

    def swap(table):
        return remote(
            grads.at[table], swapped.at[table], swap_send.at[table], swap_recv.at[table], other
        )

    def arrive(table):
        remote(
            out_ref.at[table, pl.ds(0, owners - 1)], grads.at[table, pl.ds(0, owners - 1)],
            grad_send.at[table], grad_recv.at[table], other,
        ).wait()
        swap(table).start()

    def place(table):
        swap(table).wait()
        values = jnp.concatenate(
            [grads[table].reshape(slots, width), swapped[table].reshape(slots, width)], axis=0
        )
        upper = values * high_ref[table]
        values = jnp.concatenate([values - upper, upper], axis=1)
        block = 256
        one, zero = jnp.ones((block, LANES), BF16), jnp.zeros((block, LANES), BF16)
        for start in range(0, half_rows // 2, block):
            at = (iota((block, LANES), 0) + start).astype(I16)
            hits = [
                jnp.where(
                    jnp.concatenate(
                        [place_keys[table, :, lane : lane + LANES]] * (block // 16), axis=0
                    ) == at, one, zero,
                )
                for lane in range(0, 2 * slots, LANES)
            ]
            both = jnp.dot(jnp.concatenate(hits, axis=1), values, preferred_element_type=F32)
            for part in range(2):
                summed = both[:, part * width : (part + 1) * width]
                mean = jnp.sum(summed * summed, axis=1, keepdims=True) * (1.0 / width)
                rows_at = part * (half_rows // 2) + start
                emb_rows[table, rows_at : rows_at + block, :] = summed * (
                    1.0 / (jnp.sqrt(mean) + 1e-06)
                )

    def to_plane(src_of, dst_of, send, recv):
        for step in range(1, inner):
            to = lax.rem(low + step, inner)
            remote(src_of(to), dst_of(step - 1), send, recv, (high * inner + to, core)).start()

    def to_column(src, dst, send, recv):
        for step in range(1, outer):
            to = lax.rem(high + step, outer)
            remote(src, dst, send, recv, (to * inner + low, core)).start()

    columns = ((column_s, from_column_s), (column_q, from_column_q))

    def await_all(src, dst, send, recv):
        remote(src, dst, send, recv, other).wait()

    def plane_sum(chunk):
        for at, (src, dst) in enumerate(((plane_s, from_plane_s), (plane_q, from_plane_q))):
            to_plane(
                lambda to: src.at[chunk, to], lambda slot: dst.at[chunk, slot],
                plane_send.at[at, chunk], plane_recv.at[at, chunk],
            )

    def plane_summed(chunk):
        for at, (src, dst) in enumerate(((plane_s, from_plane_s), (plane_q, from_plane_q))):
            await_all(
                src.at[chunk, pl.ds(0, inner - 1)], dst.at[chunk], plane_send.at[at, chunk],
                plane_recv.at[at, chunk],
            )

    def column_sum(chunk):
        for hub in range(2):

            @pl.when(high != half - 1 + hub)
            def _():
                for at, (src, dst) in enumerate(columns):
                    remote(
                        src.at[chunk, hub], dst.at[chunk, high], column_send.at[at, chunk],
                        column_recv.at[at, chunk], ((half - 1 + hub) * inner + low, core),
                    ).start()

    def column_summed(chunk):
        for at, (src, dst) in enumerate(columns):
            sems = column_send.at[at, chunk], column_recv.at[at, chunk], other

            @pl.when(is_hub)
            def _():
                remote(src.at[chunk, 0], dst.at[chunk, 0], *sems).wait_send()
                some = dst.at[chunk, pl.ds(0, outer - 1)]
                remote(some, some, *sems).wait_recv()

            @pl.when(jnp.logical_not(is_hub))
            def _():
                remote(src.at[chunk], src.at[chunk], *sems).wait_send()

    def column_share(chunk):
        for at, part in enumerate((share_s, share_q)):
            mine = part.at[chunk, core, low, high - (half - 1)]
            to_column(mine, mine, column_send.at[2 + at, chunk], column_recv.at[2 + at, chunk])

    def column_shared(chunk):
        for at, part in enumerate((share_s, share_q)):
            sems = column_send.at[2 + at, chunk], column_recv.at[2 + at, chunk], other

            @pl.when(is_hub)
            def _():
                some = columns[at][1].at[chunk, pl.ds(0, outer - 1)]
                remote(some, some, *sems).wait_send()
                one = part.at[chunk, core, low, 0]
                remote(one, one, *sems).wait_recv()

            @pl.when(jnp.logical_not(is_hub))
            def _():
                both = part.at[chunk, core, low]
                remote(both, both, *sems).wait_recv()

    def plane_share(chunk):
        for at, part in enumerate((share_s, share_q)):
            mine = part.at[chunk, core, low]
            to_plane(
                lambda to: mine, lambda slot: mine, plane_send.at[2 + at, chunk],
                plane_recv.at[2 + at, chunk],
            )

    def plane_shared(chunk):
        for at, part in enumerate((share_s, share_q)):
            some = part.at[chunk, core, pl.ds(0, inner - 1)]
            await_all(some, some, plane_send.at[2 + at, chunk], plane_recv.at[2 + at, chunk])

    def pair_down(chunk):
        return [
            remote(
                part.at[chunk, core], part.at[chunk, core], pair_send.at[phase, chunk],
                pair_recv.at[phase, chunk], other,
            )
            for phase, part in ((1, share_s), (2, share_q))
        ]

    def coded(values):
        most = jnp.max(jnp.abs(values), axis=0, keepdims=True)
        most = jnp.where(most < 1e-34, 0.0, most)
        code = jnp.round(values * jnp.where(most > 0.0, 32767.0 / most, 0.0))
        return code.astype(jnp.int32).astype(I16), most * (1.0 / 32767.0)

    def decoded(code, scale):
        return code.astype(jnp.int32).astype(F32) * scale

    def run(copies):
        for copy in copies:
            copy.start()

    def finish(copies):
        for copy in copies:
            copy.wait()

    def pair_step(chunk):
        pair_up(chunk).wait()
        for to in range(inner):
            values = dense_ref[chunk, core, to] + from_other[chunk, to]
            sum_pair[chunk, to] = values
            code, plane_s[chunk, to] = coded(values.reshape(2 * rows, piece))
            plane_q[chunk, to] = code.reshape(2, rows, piece)
        plane_sum(chunk)
        if chunk == CHUNKS - 1:
            extra_up.wait()
            extra_pair[...] = extra_ref[...] + extra_other[...]
            extra_plane[low] = extra_ref[...] + extra_other[...]
            to_plane(
                lambda to: extra_pair, lambda slot: extra_plane.at[low], extra_send.at[1],
                extra_recv.at[1],
            )

    def plane_step(chunk):
        plane_summed(chunk)
        part = sum_pair[chunk, low].reshape(2 * rows, piece)
        for slot in range(inner - 1):
            part = part + decoded(
                from_plane_q[chunk, slot].reshape(2 * rows, piece), from_plane_s[chunk, slot]
            )
        for to in range(2):
            values = part[to * rows : (to + 1) * rows]
            sum_plane[chunk, to] = values
            column_q[chunk, to], column_s[chunk, to] = coded(values)
        column_sum(chunk)
        if chunk == CHUNKS - 1:
            some = extra_plane.at[pl.ds(0, inner - 1)]
            await_all(some, some, extra_send.at[1], extra_recv.at[1])
            part = extra_plane[0]
            for slot in range(1, inner):
                part = part + extra_plane[slot]
            extra_sum[...] = part
            extra_column[high] = part
            to_column(extra_sum, extra_column.at[high], extra_send.at[2], extra_recv.at[2])

    def column_step(chunk):
        column_summed(chunk)

        @pl.when(is_hub)
        def _():
            hub = high - (half - 1)
            part = sum_plane[chunk, hub]
            for step in range(1, outer):
                at = lax.rem(high + step, outer)
                part = part + decoded(from_column_q[chunk, at], from_column_s[chunk, at])
            code, scale = coded(part)
            share_q[chunk, core, low, hub] = code
            share_s[chunk, core, low, hub] = scale
            column_share(chunk)

        if chunk == CHUNKS - 1:
            some = extra_column.at[pl.ds(0, outer - 1)]
            await_all(some, some, extra_send.at[2], extra_recv.at[2])
            part = extra_column[0]
            for slot in range(1, outer):
                part = part + extra_column[slot]
            small_ref[...] = part

    def share_step(chunk):
        column_shared(chunk)
        plane_share(chunk)

    def down_step(chunk):
        plane_shared(chunk)
        run(pair_down(chunk))

    def last_step(chunk):
        finish(pair_down(chunk))

    steps = {
        "weight": weight_step, "far": send_grads, "near": near_step, "pair": pair_step, "plane": plane_step, "column": column_step,
        "share": share_step, "down": down_step, "last": last_step, "arrive": arrive, "place": place,
    }
    for word in ORDER:
        with jax.named_scope(word):
            steps[word[:-1]](int(word[-1]))


ORDER = (
    "far0", "weight0", "weight1", "far1", "pair0", "pair1", "far2", "plane0", "near0",
    "plane1", "near1", "far3", "near2", "near3", "column0", "arrive0", "column1", "place0",
    "share0", "arrive1", "share1", "place1", "arrive2", "down0", "down1", "arrive3", "place2",
    "place3", "last0", "last1",
)


def write_body(
    params, sessions, rows_hbm, code_ref, scale_ref, small_ref, emb_hbm, hidden_hbm, bias_hbm,
    score_hbm, loss_hbm, hidden_ref, bias_ref, score_ref, loss_ref, row_sems, sems,
):
    copies = [
        pltpu.make_async_copy(rows_hbm.at[table], emb_hbm.at[table], row_sems.at[table])
        for table in range(rows_hbm.shape[0])
    ]
    for copy in copies:
        copy.start()
    hid = hidden_ref.shape[0]
    piece = code_ref.shape[-1]
    small = small_ref[...]
    counts = jnp.where(iota(small.shape, 0) < 2, small, 0.0)
    squares = jnp.sum(counts * counts, keepdims=True)
    for chunk in range(hid // piece):
        part = code_ref[chunk].astype(jnp.int32).astype(F32) * scale_ref[chunk]
        part = part.reshape(hid, piece)
        hidden_ref[:, chunk * piece : (chunk + 1) * piece] = part
        squares = squares + jnp.sum(part * part, keepdims=True)
    factor = 1.0 / jnp.sqrt(squares / params + 1e-06)
    hidden_ref[...] = hidden_ref[...] * factor
    bias_ref[...] = small[0:1, :] * factor
    score_ref[...] = small[1:2, :] * factor
    loss_ref[...] = small[2:3, 0:1] / sessions
    for at, (src, dst) in enumerate(
        (
            (hidden_ref, hidden_hbm), (bias_ref, bias_hbm), (score_ref, score_hbm),
            (loss_ref, loss_hbm),
        )
    ):
        copies.append(pltpu.make_async_copy(src, dst, sems.at[at]))
        copies[-1].start()
    for copy in copies:
        copy.wait()


def whole_kernel(
    tables, owner_ids, row_ids, session, relevance, logit_bias, w_hidden, bias_hidden, w_score
):
    table_count, shard_rows, width = tables.shape
    owners = lax.axis_size("table")
    imps = row_ids.shape[1]
    capacity = 2 * imps // owners
    hid = w_hidden.shape[1]
    slots = owners * capacity
    half_rows = shard_rows // 2
    inner = 1
    while inner * inner < owners:
        inner *= 2
    outer = owners // inner
    rows = hid // (4 * inner)
    piece = hid // CHUNKS
    sizes = (table_count, owners, capacity, width, half_rows, inner, outer, hid)
    dma = pltpu.SemaphoreType.DMA
    vmem = pl.BlockSpec(memory_space=pltpu.VMEM)
    hbm = pl.BlockSpec(memory_space=pltpu.HBM)
    lookups = (table_count, owners, capacity, width)
    emb_rows, codes, scales, small = pl.pallas_call(
        functools.partial(whole_body, sizes),
        out_shape=(
            jax.ShapeDtypeStruct((table_count, half_rows, width), F32),
            jax.ShapeDtypeStruct((CHUNKS, 2, inner, 2, rows, piece), I16),
            jax.ShapeDtypeStruct((CHUNKS, 2, inner, 2, 1, piece), F32),
            jax.ShapeDtypeStruct((4, hid), F32),
        ),
        in_specs=[hbm] * 9,
        out_specs=(vmem, vmem, vmem, vmem),
        scratch_shapes=[
            pltpu.VMEM(tables.shape, BF16),
            pltpu.VMEM(owner_ids.shape, jnp.int32),
            pltpu.VMEM(row_ids.shape, jnp.int32),
            pltpu.VMEM(session.shape, jnp.int32),
            pltpu.VMEM(relevance.shape, F32),
            pltpu.VMEM(logit_bias.shape, F32),
            pltpu.VMEM(w_hidden.shape, F32),
            pltpu.VMEM(bias_hidden.shape, F32),
            pltpu.VMEM(w_score.shape, F32),
            pltpu.VMEM(w_hidden.shape, BF16),
            pltpu.VMEM((LANES, imps), F32),
            pltpu.VMEM((imps, LANES), F32),
            pltpu.VMEM((owners, 1, LANES), F32),
            pltpu.VMEM((owners, 1, LANES), F32),
            pltpu.VMEM((owners, 1, LANES), F32),
            pltpu.VMEM((2 * LANES, table_count * LANES), BF16),
            pltpu.VMEM((8, 2 * LANES), BF16),
            pltpu.VMEM((slots, table_count * LANES), F32),
            pltpu.VMEM((table_count, 16, 2 * slots), I16),
            pltpu.VMEM((table_count, 2 * slots, LANES), BF16),
            pltpu.VMEM((table_count, imps, slots), BF16),
            pltpu.VMEM((table_count, slots, imps), BF16),
            pltpu.VMEM(lookups, BF16),
            pltpu.VMEM(lookups, BF16),
            pltpu.VMEM((imps, table_count * width), BF16),
            pltpu.VMEM((table_count * width, imps), BF16),
            pltpu.VMEM(lookups, BF16),
            pltpu.VMEM(lookups, BF16),
            pltpu.VMEM(lookups, BF16),
            pltpu.VMEM((CHUNKS, 2, inner, 2, rows, piece), F32),
            pltpu.VMEM((CHUNKS, inner, 2, rows, piece), F32),
            pltpu.VMEM((CHUNKS, inner, 2, rows, piece), F32),
            pltpu.VMEM((CHUNKS, inner, 2, rows, piece), I16),
            pltpu.VMEM((CHUNKS, inner, 1, piece), F32),
            pltpu.VMEM((CHUNKS, inner - 1, 2, rows, piece), I16),
            pltpu.VMEM((CHUNKS, inner - 1, 1, piece), F32),
            pltpu.VMEM((CHUNKS, 2, rows, piece), F32),
            pltpu.VMEM((CHUNKS, 2, rows, piece), I16),
            pltpu.VMEM((CHUNKS, 2, 1, piece), F32),
            pltpu.VMEM((CHUNKS, outer, rows, piece), I16),
            pltpu.VMEM((CHUNKS, outer, 1, piece), F32),
            pltpu.VMEM((4, hid), F32),
            pltpu.VMEM((4, hid), F32),
            pltpu.VMEM((inner, 4, hid), F32),
            pltpu.VMEM((outer, 4, hid), F32),
            pltpu.VMEM((4, hid), F32),
            pltpu.VMEM((4, hid), F32),
            dma((1,)), dma((8,)), dma((2,)),
            dma((table_count,)), dma((table_count,)), dma((2,)), dma((table_count,)),
            dma((table_count,)), dma((table_count,)), dma((table_count,)),
            dma((3, CHUNKS)), dma((3, CHUNKS)),
            dma((4, CHUNKS)), dma((4, CHUNKS)), dma((4, CHUNKS)), dma((4, CHUNKS)),
            dma((3,)), dma((3,)),
        ],
        compiler_params=pltpu.CompilerParams(
            collective_id=1, has_side_effects=True, vmem_limit_bytes=44 * 1024 * 1024
        ),
    )(
        *(
            pltpu.with_memory_space_constraint(operand, pltpu.HBM)
            for operand in (
                tables, owner_ids, row_ids, session, relevance, logit_bias, w_hidden, bias_hidden,
                w_score,
            )
        )
    )
    params = hid * hid + 2 * hid
    emb_step, step_hidden, step_bias, step_score, loss = pl.pallas_call(
        functools.partial(write_body, params, SESS_DEV * owners * 2),
        out_shape=(
            jax.ShapeDtypeStruct((table_count, half_rows, width), F32),
            jax.ShapeDtypeStruct((hid, hid), F32),
            jax.ShapeDtypeStruct((1, hid), F32),
            jax.ShapeDtypeStruct((1, hid), F32),
            jax.ShapeDtypeStruct((1, 1), F32),
        ),
        in_specs=[vmem] * 4,
        out_specs=(hbm,) * 5,
        scratch_shapes=[
            pltpu.VMEM((hid, hid), F32), pltpu.VMEM((1, hid), F32), pltpu.VMEM((1, hid), F32),
            pltpu.VMEM((1, 1), F32), dma((table_count,)), dma((4,)),
        ],
        compiler_params=pltpu.CompilerParams(vmem_limit_bytes=8 * 1024 * 1024),
    )(emb_rows, codes, scales, small)
    return (emb_step, step_hidden, step_bias[0], step_score[0], loss[0, 0])


def solution(mesh):
    in_specs = (
        P(None, "table", None),
        P(("table", "dp"), None, None, None),
        P(("table", "dp"), None, None),
        P(("table", "dp"), None),
        P(("table", "dp"), None),
        P(("table", "dp"), None),
        P(),
        P(),
        P(),
    )
    out_specs = (P(None, ("table", "dp"), None), P(), P(), P(), P())
    return jax.shard_map(
        on_device, mesh=mesh, in_specs=in_specs, out_specs=out_specs, check_vma=False
    )
```

```python
import jax
import jax.numpy as jnp
from jax import lax
from jax.experimental import pallas as pl
from jax.experimental.pallas import tpu as pltpu
import functools
from jax.sharding import PartitionSpec as P

SESS_DEV = 2


def silu_slope(pre_val):
    logistic = jax.nn.sigmoid(pre_val)
    return logistic * (1.0 + pre_val * (1.0 - logistic))


def session_terms(scores, session_ids, relevance, sessions):
    member = session_ids[None, :] == jnp.arange(sessions, dtype=jnp.int32)[:, None]
    highest = jnp.max(jnp.where(member, scores[None, :], -jnp.inf), axis=1)
    highest_each = jnp.sum(jnp.where(member, highest[:, None], 0.0), axis=0)
    shifted = scores - highest_each
    exponent = jnp.exp(shifted)
    totals = jnp.sum(jnp.where(member, exponent[None, :], 0.0), axis=1)
    weights = jnp.sum(jnp.where(member, relevance[None, :], 0.0), axis=1)
    total_each = jnp.sum(jnp.where(member, totals[:, None], 0.0), axis=0)
    weight_each = jnp.sum(jnp.where(member, weights[:, None], 0.0), axis=0)
    probability = exponent / total_each
    target = relevance / weight_each
    loss_sum = jnp.sum(jnp.log(totals)) - jnp.sum(target * shifted)
    return (loss_sum, probability - target)


def selector(indices, count):
    return (indices[:, None] == jnp.arange(count, dtype=jnp.int32)[None, :]).astype(jnp.bfloat16)


def pick_rows(indices, source):
    return jnp.dot(
        selector(indices, source.shape[0]), source, preferred_element_type=jnp.float32
    ).astype(jnp.bfloat16)


def place_rows(indices, values, count):
    return lax.dot_general(
        selector(indices, count),
        values,
        (((0,), (0,)), ((), ())),
        preferred_element_type=jnp.float32,
    )


def on_device(
    tables, owner_ids, row_ids, session_of, relevance, logit_bias, w_hidden, bias_hidden, w_score
):
    owners = lax.axis_size("table")
    devices = owners * lax.axis_size("dp")
    table_count, shard_rows, emb_width = tables.shape
    imp_count = row_ids.shape[2]
    capacity = 2 * imp_count // owners
    if (
        capacity % 16 == 0
        and table_count * capacity == 128
        and w_hidden.shape[0] == w_hidden.shape[1] == table_count * emb_width
        and emb_width == 128
    ):
        return whole_kernel(
            tables,
            owner_ids.reshape(table_count, 1, imp_count),
            row_ids[0],
            session_of,
            relevance,
            logit_bias,
            w_hidden,
            bias_hidden[None, :],
            w_score[None, :],
        )
    owner_now = owner_ids[0, :, :, 0]
    rows_now = row_ids[0]
    slot_total = owners * capacity
    one_hot = (owner_now[:, :, None] == jnp.arange(owners, dtype=jnp.int32)).astype(jnp.float32)
    places = jnp.arange(imp_count, dtype=jnp.int32)
    lower_tri = (places[:, None] >= places[None, :]).astype(jnp.float32)
    running = jnp.einsum("ij,tjo->tio", lower_tri, one_hot, precision=lax.Precision.HIGHEST)
    rank_in = (jnp.sum(running * one_hot, axis=2) - 1.0).astype(jnp.int32)
    slot_of = owner_now * capacity + rank_in
    slot_hot = (slot_of[:, :, None] == jnp.arange(slot_total, dtype=jnp.int32)).astype(jnp.int32)
    wanted = jnp.sum(slot_hot * rows_now[:, :, None], axis=1) + shard_rows * (
        1 - jnp.sum(slot_hot, axis=1)
    )
    requested = lax.all_to_all(
        wanted.reshape(table_count, owners, capacity),
        "table",
        split_axis=1,
        concat_axis=1,
        tiled=True,
    )
    served = lax.map(
        lambda pair: pick_rows(pair[0], pair[1]),
        (requested.reshape(table_count, slot_total), tables),
    )
    served = served.reshape(table_count, owners, capacity, emb_width)
    hidden_bf = w_hidden.astype(jnp.bfloat16)
    returned = lax.all_to_all(served, "table", split_axis=1, concat_axis=1, tiled=True).reshape(
        table_count, slot_total, emb_width
    )
    gathered = lax.map(lambda pair: pick_rows(pair[0], pair[1]), (slot_of, returned))
    inputs = jnp.transpose(gathered, (1, 0, 2)).reshape(imp_count, table_count * emb_width)
    pre_act = jnp.dot(inputs, hidden_bf, preferred_element_type=jnp.float32)
    pre_act = pre_act + bias_hidden
    hidden = jax.nn.silu(pre_act)
    scores = jnp.dot(hidden, w_score, precision=lax.Precision.HIGHEST) + logit_bias[0]
    loss_sum, score_grad = session_terms(scores, session_of[0], relevance[0], SESS_DEV)
    pre_grad = score_grad[:, None] * w_score[None, :] * silu_slope(pre_act)
    pre_grad_bf = pre_grad.astype(jnp.bfloat16)
    weight_grad = lax.dot_general(
        inputs, pre_grad_bf, (((0,), (0,)), ((), ())), preferred_element_type=jnp.float32
    )
    bias_grad = jnp.sum(pre_grad, axis=0)
    score_weight_grad = jnp.dot(score_grad, hidden, precision=lax.Precision.HIGHEST)
    input_grad = jnp.dot(pre_grad_bf, hidden_bf.T, preferred_element_type=jnp.float32).astype(
        jnp.bfloat16
    )
    input_grad = jnp.transpose(input_grad.reshape(imp_count, table_count, emb_width), (1, 0, 2))
    outgoing = lax.map(
        lambda pair: place_rows(pair[0], pair[1], slot_total).astype(jnp.bfloat16),
        (slot_of, input_grad),
    )
    incoming = lax.all_to_all(
        outgoing.reshape(table_count, owners, capacity, emb_width),
        "table",
        split_axis=1,
        concat_axis=1,
        tiled=True,
    )
    summed = lax.map(
        lambda pair: place_rows(pair[0], pair[1], shard_rows),
        (
            requested.reshape(table_count, slot_total),
            incoming.reshape(table_count, slot_total, emb_width),
        ),
    )
    own_rows = lax.psum_scatter(summed, "dp", scatter_dimension=1, tiled=True)
    emb_step = own_rows / (jnp.sqrt(jnp.mean(own_rows * own_rows, axis=2, keepdims=True)) + 1e-06)
    param_count = w_hidden.size + bias_hidden.size + w_score.size
    weight_tot, bias_tot, score_tot, loss_tot = lax.psum(
        (weight_grad, bias_grad, score_weight_grad, loss_sum), ("table", "dp")
    )
    mean_sq = (
        jnp.sum(weight_tot * weight_tot)
        + jnp.sum(bias_tot * bias_tot)
        + jnp.sum(score_tot * score_tot)
    ) / param_count
    factor = 1.0 / jnp.sqrt(mean_sq + 1e-06)
    step_hidden = weight_tot * factor
    loss = loss_tot / (SESS_DEV * devices)
    return (emb_step, step_hidden, bias_tot * factor, score_tot * factor, loss)


MESH = pl.DeviceIdType.MESH
F32, BF16, I16 = jnp.float32, jnp.bfloat16, jnp.int16
CHUNKS = 2
LANES = 128


def iota(shape, dim):
    return lax.broadcasted_iota(jnp.int32, shape, dim)


def ones_where(mask):
    return jnp.where(mask, 1.0, 0.0)


def lane_hits(key, base, blocks):
    at = [(iota((16, LANES), 1) + (base + k * LANES)).astype(I16) for k in range(blocks)]
    one, zero = jnp.ones(key.shape, BF16), jnp.zeros(key.shape, BF16)
    return jnp.concatenate(
        [
            jnp.where(key == jnp.concatenate([lanes] * (key.shape[0] // 16), axis=0), one, zero)
            for lanes in at
        ],
        axis=1,
    )


def whole_body(
    sizes, tables_hbm, owner_hbm, rows_hbm, session_hbm, relevance_hbm, place_hbm, weights_hbm,
    bias_hbm, scorer_hbm,
    emb_rows, share_q, share_s, small_ref,
    tables_ref, owner_ref, asked_rows, session_ref, relevance_ref, place_ref, weights_ref, bias_ref,
    scorer_ref, w_bf, meta_ref, columns_ref, want_ref, ids_in, ids_other, spread_ref, pack_ref,
    ids_cols, place_keys, high_ref, hot_ref, hot_rows, served, picked, gathered, inputs_t, out_ref,
    grads, swapped,
    dense_ref, from_other, sum_pair, plane_q, plane_s, from_plane_q, from_plane_s, sum_plane,
    column_q, column_s, from_column_q, from_column_s,
    extra_ref, extra_other, extra_plane, extra_column, extra_pair, extra_sum,
    load_sem, fetch_sem, want_sems, serve_send, serve_recv, ids_sems, grad_send,
    grad_recv, swap_send, swap_recv, pair_send, pair_recv, plane_send, plane_recv, column_send,
    column_recv, extra_send, extra_recv,
):
    tables, owners, capacity, width, half_rows, inner, outer, hid = sizes
    slots = owners * capacity
    imps = asked_rows.shape[1]
    shard_rows = 2 * half_rows
    me = lax.axis_index("table")
    core = lax.axis_index("dp")
    low, high = lax.rem(me, inner), me // inner
    other = (me, 1 - core)
    half = outer // 2
    is_hub = (high >= half - 1) & (high <= half)

    barrier = pltpu.get_barrier_semaphore()

    def greet(step, carry):
        pl.semaphore_signal(
            barrier, inc=1, device_id=(lax.rem(me + step, owners), core), device_id_type=MESH
        )
        return carry

    pl.semaphore_signal(barrier, inc=1, device_id=other, device_id_type=MESH)
    lax.fori_loop(1, owners, greet, 0)

    sources = [
        (owner_hbm, owner_ref), (rows_hbm, asked_rows), (session_hbm, session_ref),
        (relevance_hbm, relevance_ref), (place_hbm, place_ref), (weights_hbm, weights_ref),
        (bias_hbm, bias_ref), (scorer_hbm, scorer_ref),
    ]
    fetches = [
        pltpu.make_async_copy(src, dst, fetch_sem.at[at]) for at, (src, dst) in enumerate(sources)
    ]

    load = pltpu.make_async_copy(tables_hbm, tables_ref, load_sem.at[0])

    for fetch in fetches:
        fetch.start()
    load.start()

    def remote(src, dst, send, recv, to):
        return pltpu.make_async_remote_copy(
            src_ref=src, dst_ref=dst, send_sem=send, recv_sem=recv, device_id=to,
            device_id_type=MESH,
        )

    def to_peers(copy_to, far_too=True, near_too=True):
        def far(step, carry):
            up = (1 - high // half) * (half - 1 - 2 * (step // inner))
            plane = (1 - high // half) * half + step // inner + up
            copy_to(plane * inner + lax.rem(low + lax.rem(step, inner), inner)).start()
            return carry

        def near(step, carry):
            plane = (high // half) * half + lax.rem(lax.rem(high, half) + 1 + step // inner, half)
            copy_to(plane * inner + lax.rem(low + lax.rem(step, inner), inner)).start()
            return carry

        def level(step, carry):
            copy_to(high * inner + lax.rem(low + step, inner)).start()
            return carry

        if far_too:
            lax.fori_loop(0, half * inner, far, 0)
        if near_too:
            lax.fori_loop(0, (half - 1) * inner, near, 0)
            lax.fori_loop(1, inner, level, 0)

    for fetch in fetches[:5]:
        fetch.wait()
    asked = [ones_where(iota((owners, imps), 0) == owner_ref[table]) for table in range(tables)]
    upto = ones_where(iota((imps, imps), 0) <= iota((imps, imps), 1)).astype(BF16)
    running = jnp.dot(
        jnp.concatenate(asked, axis=0).astype(BF16), upto, preferred_element_type=F32
    )
    tops, lows, keys = [], [], []
    meta_ref[...] = jnp.zeros_like(meta_ref)
    for table in range(tables):
        rank = jnp.sum(
            asked[table] * running[table * owners : (table + 1) * owners], axis=0, keepdims=True
        ) - 1.0
        meta_ref[table : table + 1, :] = owner_ref[table].astype(F32) * capacity + rank
        code = asked_rows[table : table + 1, :] + 1
        tops.append(asked[table] * (code >> 6).astype(F32))
        lows.append(asked[table] * (code & 63).astype(F32))
        keys.append(
            ones_where(iota((LANES, imps), 0) == rank.astype(jnp.int32) + table * capacity)
        )
    codes = jnp.concatenate(
        [jnp.concatenate(tops, axis=1), jnp.concatenate(lows, axis=1)], axis=0
    ).astype(BF16)
    packed = lax.dot_general(
        codes, jnp.concatenate(keys, axis=1).astype(BF16), (((1,), (1,)), ((), ())),
        preferred_element_type=F32,
    )
    want_ref[...] = (packed[:owners] * 64.0 + packed[owners:]).reshape(owners, 1, LANES)
    with jax.named_scope("barrier_wait"):
        pl.semaphore_wait(barrier, owners)

    to_peers(
        lambda peer: remote(
            want_ref.at[peer], ids_in.at[me], want_sems.at[0], want_sems.at[1], (peer, core)
        )
    )
    ids_in[me] = want_ref[me]

    meta_ref[tables : tables + 1, :] = session_ref[...].astype(F32)
    meta_ref[tables + 1 : tables + 2, :] = relevance_ref[...]
    meta_ref[tables + 2 : tables + 3, :] = place_ref[...]
    columns_ref[...] = meta_ref[...].T
    block_of = lax.rem(iota((2 * LANES, tables * LANES), 0), LANES) // capacity
    scale = jnp.where(iota((2 * LANES, tables * LANES), 0) < LANES, 64.0, 1.0)
    spread_ref[...] = jnp.where(
        block_of == iota((2 * LANES, tables * LANES), 1) // LANES, scale, 0.0
    ).astype(BF16)
    pack_at = iota((8, 2 * LANES), 1)
    pack_ref[...] = jnp.where(
        lax.rem(pack_at, LANES) // capacity == iota((8, 2 * LANES), 0),
        jnp.where(pack_at < LANES, 64.0, 1.0), 0.0,
    ).astype(BF16)
    for fetch in fetches[5:]:
        fetch.wait()
    w_bf[...] = weights_ref[...].astype(BF16)

    def expand(ids):
        got = ids[...]
        top = jnp.floor(got * (1.0 / 64.0))
        shape = (owners, capacity, LANES)
        keep = lax.rem(iota(shape, 2), capacity) == iota(shape, 1)
        parts = [
            jnp.where(keep, jnp.broadcast_to(part, shape), 0.0).astype(BF16).reshape(slots, LANES)
            for part in (top, got - top * 64.0)
        ]
        return jnp.concatenate(parts, axis=1)

    def columns_of(codes):
        return jnp.dot(codes, spread_ref[...], preferred_element_type=F32)

    with jax.named_scope("ids_wait"):
        remote(
            want_ref.at[pl.ds(0, owners - 1)], ids_in.at[pl.ds(0, owners - 1)], want_sems.at[0],
            want_sems.at[1], other,
        ).wait()
    ids_copy = remote(ids_in, ids_other, ids_sems.at[0], ids_sems.at[1], other)
    ids_copy.start()
    codes_mine = expand(ids_in)
    ids_cols[...] = columns_of(codes_mine)

    def pick(table, first, count):
        code = ids_cols[
            pl.ds(pl.multiple_of(first * capacity, capacity), count * capacity),
            table * LANES : (table + 1) * LANES,
        ]
        upper = code > half_rows
        key = jnp.where(upper, code - (half_rows + 1.0), code - 1.0).astype(jnp.int32).astype(I16)
        both = jnp.zeros((count * capacity, 2 * width), F32)
        depth = 256
        for at in range(0, half_rows, depth):
            rows = jnp.concatenate(
                [
                    tables_ref[table, at : at + depth, :],
                    tables_ref[table, half_rows + at : half_rows + at + depth, :],
                ],
                axis=1,
            )
            both = both + jnp.dot(
                lane_hits(key, at, depth // LANES), rows, preferred_element_type=F32
            )
        served[table, pl.ds(first, count)] = (
            jnp.where(upper, both[:, width:], both[:, :width])
            .astype(BF16)
            .reshape(count, capacity, width)
        )

    def serve(table, far_too, near_too):
        to_peers(
            lambda peer: remote(
                served.at[table, peer], picked.at[table, me], serve_send.at[table],
                serve_recv.at[table], (peer, core),
            ),
            far_too, near_too,
        )

    with jax.named_scope("pick"):
        load.wait()
        side = high // half
        part = owners // 2
        pick(0, (1 - side) * part, part)
        serve(0, True, False)
        pick(0, side * part, part)
        serve(0, False, True)
        for table in range(1, tables):
            pick(table, 0, owners)
            serve(table, True, True)
        for table in range(tables):
            picked[table, me] = served[table, me]

    with jax.named_scope("prep"):
        for table in range(tables):
            hot_ref[table] = ones_where(
                iota((imps, slots), 1) == columns_ref[:, table : table + 1].astype(jnp.int32)
            ).astype(BF16)
            hot_rows[table] = ones_where(
                iota((slots, imps), 0) == meta_ref[table : table + 1, :].astype(jnp.int32)
            ).astype(BF16)
        quarter = half_rows // 2
        first = (core * half_rows).astype(F32)

        def place_prep(codes, columns, at):
            lanes = lax.dot_general(
                pack_ref[...], codes, (((1,), (1,)), ((), ())), preferred_element_type=F32
            ) - (first + 1.0)
            inside = (lanes >= 0.0) & (lanes < half_rows)
            key = jnp.where(lanes >= quarter, lanes - quarter, lanes)
            key = jnp.where(inside, key, -1.0).astype(jnp.int32)
            for table in range(tables):
                place_keys[table, :, at : at + slots] = jnp.broadcast_to(
                    key[table : table + 1, :], (16, slots)
                ).astype(I16)
                column = columns[:, table * LANES : (table + 1) * LANES]
                high_ref[table, at : at + slots, :] = ones_where(
                    column > first + quarter
                ).astype(BF16)

        place_prep(codes_mine, ids_cols[...], 0)
        ids_copy.wait()
        codes_theirs = expand(ids_other)
        place_prep(codes_theirs, columns_of(codes_theirs), slots)

    session = columns_ref[:, tables : tables + 1].astype(jnp.int32)
    relevance = columns_ref[:, tables + 1 : tables + 2]

    def of_session(values, reduce, fill):
        found = [
            reduce(jnp.where(session == at, values, fill), axis=0, keepdims=True)
            for at in range(SESS_DEV)
        ]
        each = jnp.broadcast_to(found[-1], values.shape)
        for at in range(SESS_DEV - 1):
            each = jnp.where(session == at, found[at], each)
        return found, each

    target = relevance / of_session(relevance, jnp.sum, 0.0)[1]
    for table in range(tables):
        with jax.named_scope(f"rows_wait{table}"):
            remote(
                served.at[table, pl.ds(0, owners - 1)], picked.at[table, pl.ds(0, owners - 1)],
                serve_send.at[table], serve_recv.at[table], other,
            ).wait()
        own = jnp.dot(
            hot_ref[table], picked[table].reshape(slots, width), preferred_element_type=F32
        )
        gathered[:, table * width : (table + 1) * width] = own.astype(BF16)
        inputs_t[table * width : (table + 1) * width, :] = own.T.astype(BF16)
    with jax.named_scope("dense"):
        pre_act = jnp.dot(gathered[...], w_bf[...], preferred_element_type=F32) + bias_ref[...]
        logistic = 1.0 / (1.0 + jnp.exp(-pre_act))
        hidden = pre_act * logistic
        scores = jnp.sum(hidden * scorer_ref[...], axis=1, keepdims=True)
        scores = scores + columns_ref[:, tables + 2 : tables + 3]
        shifted = scores - of_session(scores, jnp.max, -jnp.inf)[1]
        exponent = jnp.exp(shifted)
        sums, sum_each = of_session(exponent, jnp.sum, 0.0)
        loss_sum = sum(jnp.log(value) for value in sums) - jnp.sum(target * shifted, keepdims=True)
        score_grad = exponent / sum_each - target
        pre_grad = score_grad * scorer_ref[...] * (logistic * (1.0 + pre_act * (1.0 - logistic)))
        pre_grad_bf = pre_grad.astype(BF16)
    piece, rows = hid // CHUNKS, hid // (4 * inner)

    def pair_up(chunk):
        return remote(
            dense_ref.at[chunk, 1 - core], from_other.at[chunk], pair_send.at[0, chunk],
            pair_recv.at[0, chunk], other,
        )

    extra_up = remote(extra_ref, extra_other, extra_send.at[0], extra_recv.at[0], other)

    def weight_step(chunk):
        dense_ref[chunk] = jnp.dot(
            inputs_t[...], pre_grad_bf[:, chunk * piece : (chunk + 1) * piece],
            preferred_element_type=F32,
        ).reshape(dense_ref.shape[1:])
        pair_up(chunk).start()
        if chunk == CHUNKS - 1:
            extra_ref[...] = jnp.zeros_like(extra_ref)
            extra_ref[0:1, :] = jnp.sum(pre_grad, axis=0, keepdims=True)
            extra_ref[1:2, :] = jnp.sum(score_grad * hidden, axis=0, keepdims=True)
            extra_ref[2:3, :] = jnp.broadcast_to(loss_sum, (1, hid))
            extra_up.start()

    def give(table, far_too, near_too):
        to_peers(
            lambda peer: remote(
                out_ref.at[table, peer], grads.at[table, me], grad_send.at[table],
                grad_recv.at[table], (peer, core),
            ),
            far_too, near_too,
        )

    def near_step(table):
        give(table, False, True)

    def send_grads(table):
        input_grad = lax.dot_general(
            pre_grad_bf, w_bf[table * width : (table + 1) * width, :], (((1,), (1,)), ((), ())),
            preferred_element_type=F32,
        ).astype(BF16)
        out_ref[table] = jnp.dot(
            hot_rows[table], input_grad, preferred_element_type=F32
        ).astype(BF16).reshape(owners, capacity, width)
        grads[table, me] = out_ref[table, me]
        give(table, True, False)

    def swap(table):
        return remote(
            grads.at[table], swapped.at[table], swap_send.at[table], swap_recv.at[table], other
        )

    def arrive(table):
        remote(
            out_ref.at[table, pl.ds(0, owners - 1)], grads.at[table, pl.ds(0, owners - 1)],
            grad_send.at[table], grad_recv.at[table], other,
        ).wait()
        swap(table).start()

    def place(table):
        swap(table).wait()
        values = jnp.concatenate(
            [grads[table].reshape(slots, width), swapped[table].reshape(slots, width)], axis=0
        )
        upper = values * high_ref[table]
        values = jnp.concatenate([values - upper, upper], axis=1)
        block = 256
        one, zero = jnp.ones((block, LANES), BF16), jnp.zeros((block, LANES), BF16)
        for start in range(0, half_rows // 2, block):
            at = (iota((block, LANES), 0) + start).astype(I16)
            hits = [
                jnp.where(
                    jnp.concatenate(
                        [place_keys[table, :, lane : lane + LANES]] * (block // 16), axis=0
                    ) == at, one, zero,
                )
                for lane in range(0, 2 * slots, LANES)
            ]
            both = jnp.dot(jnp.concatenate(hits, axis=1), values, preferred_element_type=F32)
            for part in range(2):
                summed = both[:, part * width : (part + 1) * width]
                mean = jnp.sum(summed * summed, axis=1, keepdims=True) * (1.0 / width)
                rows_at = part * (half_rows // 2) + start
                emb_rows[table, rows_at : rows_at + block, :] = summed * (
                    1.0 / (jnp.sqrt(mean) + 1e-06)
                )

    def to_plane(src_of, dst_of, send, recv):
        for step in range(1, inner):
            to = lax.rem(low + step, inner)
            remote(src_of(to), dst_of(step - 1), send, recv, (high * inner + to, core)).start()

    def to_column(src, dst, send, recv):
        for step in range(1, outer):
            to = lax.rem(high + step, outer)
            remote(src, dst, send, recv, (to * inner + low, core)).start()

    columns = ((column_s, from_column_s), (column_q, from_column_q))

    def await_all(src, dst, send, recv):
        remote(src, dst, send, recv, other).wait()

    def plane_sum(chunk):
        for at, (src, dst) in enumerate(((plane_s, from_plane_s), (plane_q, from_plane_q))):
            to_plane(
                lambda to: src.at[chunk, to], lambda slot: dst.at[chunk, slot],
                plane_send.at[at, chunk], plane_recv.at[at, chunk],
            )

    def plane_summed(chunk):
        for at, (src, dst) in enumerate(((plane_s, from_plane_s), (plane_q, from_plane_q))):
            await_all(
                src.at[chunk, pl.ds(0, inner - 1)], dst.at[chunk], plane_send.at[at, chunk],
                plane_recv.at[at, chunk],
            )

    def column_sum(chunk):
        for hub in range(2):

            @pl.when(high != half - 1 + hub)
            def _():
                for at, (src, dst) in enumerate(columns):
                    remote(
                        src.at[chunk, hub], dst.at[chunk, high], column_send.at[at, chunk],
                        column_recv.at[at, chunk], ((half - 1 + hub) * inner + low, core),
                    ).start()

    def column_summed(chunk):
        for at, (src, dst) in enumerate(columns):
            sems = column_send.at[at, chunk], column_recv.at[at, chunk], other

            @pl.when(is_hub)
            def _():
                remote(src.at[chunk, 0], dst.at[chunk, 0], *sems).wait_send()
                some = dst.at[chunk, pl.ds(0, outer - 1)]
                remote(some, some, *sems).wait_recv()

            @pl.when(jnp.logical_not(is_hub))
            def _():
                remote(src.at[chunk], src.at[chunk], *sems).wait_send()

    def column_share(chunk):
        for at, part in enumerate((share_s, share_q)):
            mine = part.at[chunk, core, low, high - (half - 1)]
            to_column(mine, mine, column_send.at[2 + at, chunk], column_recv.at[2 + at, chunk])

    def column_shared(chunk):
        for at, part in enumerate((share_s, share_q)):
            sems = column_send.at[2 + at, chunk], column_recv.at[2 + at, chunk], other

            @pl.when(is_hub)
            def _():
                some = columns[at][1].at[chunk, pl.ds(0, outer - 1)]
                remote(some, some, *sems).wait_send()
                one = part.at[chunk, core, low, 0]
                remote(one, one, *sems).wait_recv()

            @pl.when(jnp.logical_not(is_hub))
            def _():
                both = part.at[chunk, core, low]
                remote(both, both, *sems).wait_recv()

    def plane_share(chunk):
        for at, part in enumerate((share_s, share_q)):
            mine = part.at[chunk, core, low]
            to_plane(
                lambda to: mine, lambda slot: mine, plane_send.at[2 + at, chunk],
                plane_recv.at[2 + at, chunk],
            )

    def plane_shared(chunk):
        for at, part in enumerate((share_s, share_q)):
            some = part.at[chunk, core, pl.ds(0, inner - 1)]
            await_all(some, some, plane_send.at[2 + at, chunk], plane_recv.at[2 + at, chunk])

    def pair_down(chunk):
        return [
            remote(
                part.at[chunk, core], part.at[chunk, core], pair_send.at[phase, chunk],
                pair_recv.at[phase, chunk], other,
            )
            for phase, part in ((1, share_s), (2, share_q))
        ]

    def coded(values):
        most = jnp.max(jnp.abs(values), axis=0, keepdims=True)
        most = jnp.where(most < 1e-34, 0.0, most)
        code = jnp.round(values * jnp.where(most > 0.0, 32767.0 / most, 0.0))
        return code.astype(jnp.int32).astype(I16), most * (1.0 / 32767.0)

    def decoded(code, scale):
        return code.astype(jnp.int32).astype(F32) * scale

    def run(copies):
        for copy in copies:
            copy.start()

    def finish(copies):
        for copy in copies:
            copy.wait()

    def pair_step(chunk):
        pair_up(chunk).wait()
        for to in range(inner):
            values = dense_ref[chunk, core, to] + from_other[chunk, to]
            sum_pair[chunk, to] = values
            code, plane_s[chunk, to] = coded(values.reshape(2 * rows, piece))
            plane_q[chunk, to] = code.reshape(2, rows, piece)
        plane_sum(chunk)
        if chunk == CHUNKS - 1:
            extra_up.wait()
            extra_pair[...] = extra_ref[...] + extra_other[...]
            extra_plane[low] = extra_ref[...] + extra_other[...]
            to_plane(
                lambda to: extra_pair, lambda slot: extra_plane.at[low], extra_send.at[1],
                extra_recv.at[1],
            )

    def plane_step(chunk):
        plane_summed(chunk)
        part = sum_pair[chunk, low].reshape(2 * rows, piece)
        for slot in range(inner - 1):
            part = part + decoded(
                from_plane_q[chunk, slot].reshape(2 * rows, piece), from_plane_s[chunk, slot]
            )
        for to in range(2):
            values = part[to * rows : (to + 1) * rows]
            sum_plane[chunk, to] = values
            column_q[chunk, to], column_s[chunk, to] = coded(values)
        column_sum(chunk)
        if chunk == CHUNKS - 1:
            some = extra_plane.at[pl.ds(0, inner - 1)]
            await_all(some, some, extra_send.at[1], extra_recv.at[1])
            part = extra_plane[0]
            for slot in range(1, inner):
                part = part + extra_plane[slot]
            extra_sum[...] = part
            extra_column[high] = part
            to_column(extra_sum, extra_column.at[high], extra_send.at[2], extra_recv.at[2])

    def column_step(chunk):
        column_summed(chunk)

        @pl.when(is_hub)
        def _():
            hub = high - (half - 1)
            part = sum_plane[chunk, hub]
            for step in range(1, outer):
                at = lax.rem(high + step, outer)
                part = part + decoded(from_column_q[chunk, at], from_column_s[chunk, at])
            code, scale = coded(part)
            share_q[chunk, core, low, hub] = code
            share_s[chunk, core, low, hub] = scale
            column_share(chunk)

        if chunk == CHUNKS - 1:
            some = extra_column.at[pl.ds(0, outer - 1)]
            await_all(some, some, extra_send.at[2], extra_recv.at[2])
            part = extra_column[0]
            for slot in range(1, outer):
                part = part + extra_column[slot]
            small_ref[...] = part

    def share_step(chunk):
        column_shared(chunk)
        plane_share(chunk)

    def down_step(chunk):
        plane_shared(chunk)
        run(pair_down(chunk))

    def last_step(chunk):
        finish(pair_down(chunk))

    steps = {
        "weight": weight_step, "far": send_grads, "near": near_step, "pair": pair_step, "plane": plane_step, "column": column_step,
        "share": share_step, "down": down_step, "last": last_step, "arrive": arrive, "place": place,
    }
    for word in ORDER:
        with jax.named_scope(word):
            steps[word[:-1]](int(word[-1]))


ORDER = (
    "far0", "weight0", "weight1", "far1", "pair0", "pair1", "far2", "plane0", "near0", "near1",
    "plane1", "far3", "near2", "near3", "column0", "arrive0", "column1", "arrive1", "place0",
    "share0", "arrive2", "share1", "place1", "arrive3", "down0", "place2", "down1", "place3",
    "last0", "last1",
)


def write_body(
    params, sessions, rows_hbm, code_ref, scale_ref, small_ref, emb_hbm, hidden_hbm, bias_hbm,
    score_hbm, loss_hbm, hidden_ref, bias_ref, score_ref, loss_ref, row_sems, sems,
):
    copies = [
        pltpu.make_async_copy(rows_hbm.at[table], emb_hbm.at[table], row_sems.at[table])
        for table in range(rows_hbm.shape[0])
    ]
    for copy in copies:
        copy.start()
    hid = hidden_ref.shape[0]
    piece = code_ref.shape[-1]
    small = small_ref[...]
    counts = jnp.where(iota(small.shape, 0) < 2, small, 0.0)
    squares = jnp.sum(counts * counts, keepdims=True)
    for chunk in range(hid // piece):
        part = code_ref[chunk].astype(jnp.int32).astype(F32) * scale_ref[chunk]
        part = part.reshape(hid, piece)
        hidden_ref[:, chunk * piece : (chunk + 1) * piece] = part
        squares = squares + jnp.sum(part * part, keepdims=True)
    factor = 1.0 / jnp.sqrt(squares / params + 1e-06)
    hidden_ref[...] = hidden_ref[...] * factor
    bias_ref[...] = small[0:1, :] * factor
    score_ref[...] = small[1:2, :] * factor
    loss_ref[...] = small[2:3, 0:1] / sessions
    for at, (src, dst) in enumerate(
        (
            (hidden_ref, hidden_hbm), (bias_ref, bias_hbm), (score_ref, score_hbm),
            (loss_ref, loss_hbm),
        )
    ):
        copies.append(pltpu.make_async_copy(src, dst, sems.at[at]))
        copies[-1].start()
    for copy in copies:
        copy.wait()


def whole_kernel(
    tables, owner_ids, row_ids, session, relevance, logit_bias, w_hidden, bias_hidden, w_score
):
    table_count, shard_rows, width = tables.shape
    owners = lax.axis_size("table")
    imps = row_ids.shape[1]
    capacity = 2 * imps // owners
    hid = w_hidden.shape[1]
    slots = owners * capacity
    half_rows = shard_rows // 2
    inner = 1
    while inner * inner < owners:
        inner *= 2
    outer = owners // inner
    rows = hid // (4 * inner)
    piece = hid // CHUNKS
    sizes = (table_count, owners, capacity, width, half_rows, inner, outer, hid)
    dma = pltpu.SemaphoreType.DMA
    vmem = pl.BlockSpec(memory_space=pltpu.VMEM)
    hbm = pl.BlockSpec(memory_space=pltpu.HBM)
    lookups = (table_count, owners, capacity, width)
    emb_rows, codes, scales, small = pl.pallas_call(
        functools.partial(whole_body, sizes),
        out_shape=(
            jax.ShapeDtypeStruct((table_count, half_rows, width), F32),
            jax.ShapeDtypeStruct((CHUNKS, 2, inner, 2, rows, piece), I16),
            jax.ShapeDtypeStruct((CHUNKS, 2, inner, 2, 1, piece), F32),
            jax.ShapeDtypeStruct((4, hid), F32),
        ),
        in_specs=[hbm] * 9,
        out_specs=(vmem, vmem, vmem, vmem),
        scratch_shapes=[
            pltpu.VMEM(tables.shape, BF16),
            pltpu.VMEM(owner_ids.shape, jnp.int32),
            pltpu.VMEM(row_ids.shape, jnp.int32),
            pltpu.VMEM(session.shape, jnp.int32),
            pltpu.VMEM(relevance.shape, F32),
            pltpu.VMEM(logit_bias.shape, F32),
            pltpu.VMEM(w_hidden.shape, F32),
            pltpu.VMEM(bias_hidden.shape, F32),
            pltpu.VMEM(w_score.shape, F32),
            pltpu.VMEM(w_hidden.shape, BF16),
            pltpu.VMEM((LANES, imps), F32),
            pltpu.VMEM((imps, LANES), F32),
            pltpu.VMEM((owners, 1, LANES), F32),
            pltpu.VMEM((owners, 1, LANES), F32),
            pltpu.VMEM((owners, 1, LANES), F32),
            pltpu.VMEM((2 * LANES, table_count * LANES), BF16),
            pltpu.VMEM((8, 2 * LANES), BF16),
            pltpu.VMEM((slots, table_count * LANES), F32),
            pltpu.VMEM((table_count, 16, 2 * slots), I16),
            pltpu.VMEM((table_count, 2 * slots, LANES), BF16),
            pltpu.VMEM((table_count, imps, slots), BF16),
            pltpu.VMEM((table_count, slots, imps), BF16),
            pltpu.VMEM(lookups, BF16),
            pltpu.VMEM(lookups, BF16),
            pltpu.VMEM((imps, table_count * width), BF16),
            pltpu.VMEM((table_count * width, imps), BF16),
            pltpu.VMEM(lookups, BF16),
            pltpu.VMEM(lookups, BF16),
            pltpu.VMEM(lookups, BF16),
            pltpu.VMEM((CHUNKS, 2, inner, 2, rows, piece), F32),
            pltpu.VMEM((CHUNKS, inner, 2, rows, piece), F32),
            pltpu.VMEM((CHUNKS, inner, 2, rows, piece), F32),
            pltpu.VMEM((CHUNKS, inner, 2, rows, piece), I16),
            pltpu.VMEM((CHUNKS, inner, 1, piece), F32),
            pltpu.VMEM((CHUNKS, inner - 1, 2, rows, piece), I16),
            pltpu.VMEM((CHUNKS, inner - 1, 1, piece), F32),
            pltpu.VMEM((CHUNKS, 2, rows, piece), F32),
            pltpu.VMEM((CHUNKS, 2, rows, piece), I16),
            pltpu.VMEM((CHUNKS, 2, 1, piece), F32),
            pltpu.VMEM((CHUNKS, outer, rows, piece), I16),
            pltpu.VMEM((CHUNKS, outer, 1, piece), F32),
            pltpu.VMEM((4, hid), F32),
            pltpu.VMEM((4, hid), F32),
            pltpu.VMEM((inner, 4, hid), F32),
            pltpu.VMEM((outer, 4, hid), F32),
            pltpu.VMEM((4, hid), F32),
            pltpu.VMEM((4, hid), F32),
            dma((1,)), dma((8,)), dma((2,)),
            dma((table_count,)), dma((table_count,)), dma((2,)), dma((table_count,)),
            dma((table_count,)), dma((table_count,)), dma((table_count,)),
            dma((3, CHUNKS)), dma((3, CHUNKS)),
            dma((4, CHUNKS)), dma((4, CHUNKS)), dma((4, CHUNKS)), dma((4, CHUNKS)),
            dma((3,)), dma((3,)),
        ],
        compiler_params=pltpu.CompilerParams(
            collective_id=1, has_side_effects=True, vmem_limit_bytes=44 * 1024 * 1024
        ),
    )(
        *(
            pltpu.with_memory_space_constraint(operand, pltpu.HBM)
            for operand in (
                tables, owner_ids, row_ids, session, relevance, logit_bias, w_hidden, bias_hidden,
                w_score,
            )
        )
    )
    params = hid * hid + 2 * hid
    emb_step, step_hidden, step_bias, step_score, loss = pl.pallas_call(
        functools.partial(write_body, params, SESS_DEV * owners * 2),
        out_shape=(
            jax.ShapeDtypeStruct((table_count, half_rows, width), F32),
            jax.ShapeDtypeStruct((hid, hid), F32),
            jax.ShapeDtypeStruct((1, hid), F32),
            jax.ShapeDtypeStruct((1, hid), F32),
            jax.ShapeDtypeStruct((1, 1), F32),
        ),
        in_specs=[vmem] * 4,
        out_specs=(hbm,) * 5,
        scratch_shapes=[
            pltpu.VMEM((hid, hid), F32), pltpu.VMEM((1, hid), F32), pltpu.VMEM((1, hid), F32),
            pltpu.VMEM((1, 1), F32), dma((table_count,)), dma((4,)),
        ],
        compiler_params=pltpu.CompilerParams(vmem_limit_bytes=8 * 1024 * 1024),
    )(emb_rows, codes, scales, small)
    return (emb_step, step_hidden, step_bias[0], step_score[0], loss[0, 0])


def solution(mesh):
    in_specs = (
        P(None, "table", None),
        P(("table", "dp"), None, None, None),
        P(("table", "dp"), None, None),
        P(("table", "dp"), None),
        P(("table", "dp"), None),
        P(("table", "dp"), None),
        P(),
        P(),
        P(),
    )
    out_specs = (P(None, ("table", "dp"), None), P(), P(), P(), P())
    return jax.shard_map(
        on_device, mesh=mesh, in_specs=in_specs, out_specs=out_specs, check_vma=False
    )
```
